256 devices in a mesh: head: 4 (over z_hi, core), ctx: 64 (over y, z_lo, x).
Axes of the slice: x: 4, y: 4, z: 8 (z_hi: 2, z_lo: 4; z = z_hi * 4 + z_lo), core: 2. Of those that a mesh axis runs over, the one named last changes fastest.
Arguments:
- queries: bfloat16 [32768, 4096], P(('ctx', 'head')), may hold values from -66 to 66
- keys: bfloat16 [32768, 4096], P(('ctx', 'head')), may hold values from -6.6 to 6.6
- values: bfloat16 [32768, 4096], P(('ctx', 'head')), may hold values from -10 to 10
- w_gate: bfloat16 [8, 512, 512], P('head'), may hold values from -0.25 to 0.25
- w_up: bfloat16 [8, 512, 512], P('head'), may hold values from -0.25 to 0.25
- w_out: bfloat16 [8, 512, 512], P('head'), may hold values from -0.25 to 0.25
Outputs:
- mixed: bfloat16 [32768, 4096], P(('ctx', 'head'))
The draws below stay inside these ranges and needn't reach their ends.
All inputs are finite; a program needn't handle non-finite values.
Results may differ from the reference program's by a relative error of at most 0.0072.
Values may be sent and summed in bfloat16 or wider, within the bound.
A program may use at most 128 MiB of HBM per device.

```python
import jax
import jax.numpy as jnp
from jax import lax

HEADS = 8
HD = 512
WIN = 512
TOK_DEV = 128
TOKENS = 32768
N_HEAD = 4


def aligned_keys(key):
    drawn_keys = jnp.clip(jax.random.normal(jax.random.fold_in(key, 11), (TOKENS, HEADS * HD), jnp.float32), -6.0, 6.0)
    jitter = jnp.clip(jax.random.normal(jax.random.fold_in(key, 12), (TOKENS, HEADS * HD), jnp.float32), -6.0, 6.0)
    position = jnp.arange(TOKENS, dtype=jnp.int32)[:, None]
    follower = jnp.roll(drawn_keys, 1, axis=0) + 0.1 * jitter
    return jnp.where(position % 61 == 1, follower, drawn_keys)


def draw_keys(key, part):
    return aligned_keys(key).astype(jnp.bfloat16)


def draw_queries(key, part):
    fresh = jnp.clip(jax.random.normal(jax.random.fold_in(key, 13), (TOKENS, HEADS * HD), jnp.float32), -6.0, 6.0)
    return fresh.astype(jnp.bfloat16)


def draw_values(key, part):
    position = jnp.arange(TOKENS, dtype=jnp.float32)[:, None]
    growth = 0.5 + position / TOKENS
    fresh = jnp.clip(jax.random.normal(jax.random.fold_in(key, 21), (TOKENS, HEADS * HD), jnp.float32), -6.0, 6.0)
    return (fresh * growth).astype(jnp.bfloat16)


def block_levels(stream_key, extent, pieces, smallest, top_value):
    factor_of, own = 1.0, jax.random.fold_in(stream_key, 6)
    for dim, blocks in pieces:
        draws = jnp.exp(jax.random.uniform(jax.random.fold_in(own, dim), (blocks,), jnp.float32, smallest / len(pieces), top_value / len(pieces)))
        factor_of = factor_of * jnp.repeat(draws, extent[dim] // blocks).reshape([-1 if axis == dim else 1 for axis in range(len(extent))])
    return factor_of


def centred(own_key, extent, deviation, most, shards=(), held_as=jnp.bfloat16):
    gain = block_levels(own_key, extent, shards, -0.22, 0.18) if shards else 1.0
    drawn = jax.random.normal(own_key, extent, jnp.float32) * deviation * gain
    return jnp.minimum(jnp.maximum(drawn, -most), most).astype(held_as)


def setup_inputs(seed: int = 0) -> dict:
    arg_keys = jax.random.split(jax.random.key(seed), 7)
    return {
        "queries": draw_queries(jax.random.fold_in(arg_keys[6], 71), 0),
        "keys": draw_keys(jax.random.fold_in(arg_keys[6], 71), 0),
        "values": draw_values(jax.random.fold_in(arg_keys[6], 71), 0),
        "w_gate": centred(arg_keys[3], (HEADS, HD, HD), HD ** -0.5, 0.25, ((0, 4),)),
        "w_up": centred(arg_keys[4], (HEADS, HD, HD), HD ** -0.5, 0.25, ((0, 4),)),
        "w_out": centred(arg_keys[5], (HEADS, HD, HD), HD ** -0.5, 0.25, ((0, 4),)),
    }


step_size = 0.02
epsilon = 1e-06

def silu_pair(inputs):
    sigmoid = jax.nn.sigmoid(inputs)
    return (inputs * sigmoid, sigmoid * (1.0 + inputs * (1.0 - sigmoid)))

def window_block(query_block, key_block, value_block, first_row):
    block_rows = query_block.shape[0]
    key_span = key_block.shape[0]
    scores = jnp.einsum('qhd,khd->hqk', query_block.astype(jnp.float32), key_block.astype(jnp.float32)) * HD ** (-0.5)
    query_place = first_row + jnp.arange(block_rows, dtype=jnp.int32)
    key_place = first_row - WIN + jnp.arange(key_span, dtype=jnp.int32)
    distance = query_place[:, None] - key_place[None, :]
    allowed = (jnp.abs(distance) <= WIN) & (key_place[None, :] >= 0) & (key_place[None, :] < TOKENS)
    masked = jnp.where(allowed[None], scores, -1e+30)
    largest = lax.optimization_barrier(jnp.max(masked, axis=2, keepdims=True))
    weights = jnp.where(allowed[None], jnp.exp(masked - largest), 0.0)
    weights = (weights / lax.optimization_barrier(jnp.sum(weights, axis=2, keepdims=True))).astype(jnp.bfloat16)
    return jnp.einsum('hqk,khd->qhd', weights.astype(jnp.float32), value_block.astype(jnp.float32))

def window_attention(queries, keys, values):
    block_rows = N_HEAD * TOK_DEV
    block_count = TOKENS // block_rows
    key_padded = jnp.pad(keys, ((WIN, WIN), (0, 0)))
    value_padded = jnp.pad(values, ((WIN, WIN), (0, 0)))

    def one_block(index):
        first_row = (index * block_rows).astype(jnp.int32)
        query_block = lax.dynamic_slice_in_dim(queries, first_row, block_rows, 0).reshape(block_rows, HEADS, HD)
        key_block = lax.dynamic_slice_in_dim(key_padded, first_row, block_rows + 2 * WIN, 0).reshape(block_rows + 2 * WIN, HEADS, HD)
        value_block = lax.dynamic_slice_in_dim(value_padded, first_row, block_rows + 2 * WIN, 0).reshape(block_rows + 2 * WIN, HEADS, HD)
        return window_block(query_block, key_block, value_block, first_row)
    result = lax.map(one_block, jnp.arange(block_count, dtype=jnp.int32))
    return result.reshape(TOKENS, HEADS * HD)

def fast_weight(query_head, key_head, value_head, gate_head, up_head, out_head):
    gate_pre = jnp.dot(key_head, gate_head, preferred_element_type=jnp.float32)
    up_pre = jnp.dot(key_head, up_head, preferred_element_type=jnp.float32)
    active, slopes = silu_pair(gate_pre)
    hidden = (active * up_pre).astype(jnp.bfloat16)
    backward = -jnp.dot(value_head, out_head.T, preferred_element_type=jnp.float32)
    gate_input = (backward * up_pre * slopes).astype(jnp.bfloat16)
    up_input = (backward * active).astype(jnp.bfloat16)
    grad_gate = jnp.dot(key_head.T, gate_input, preferred_element_type=jnp.float32)
    grad_up = jnp.dot(key_head.T, up_input, preferred_element_type=jnp.float32)
    grad_out = -jnp.dot(hidden.T, value_head, preferred_element_type=jnp.float32)
    updated = []
    for gradient, weight in ((grad_gate, gate_head), (grad_up, up_head), (grad_out, out_head)):
        inverse = lax.rsqrt(jnp.mean(gradient * gradient) + epsilon)
        updated.append((weight.astype(jnp.float32) - step_size * inverse * gradient).astype(jnp.bfloat16))
    query_gate = jnp.dot(query_head, updated[0], preferred_element_type=jnp.float32)
    query_up = jnp.dot(query_head, updated[1], preferred_element_type=jnp.float32)
    query_hidden = (jax.nn.silu(query_gate) * query_up).astype(jnp.bfloat16)
    return jnp.dot(query_hidden, updated[2], preferred_element_type=jnp.float32)

def reference(queries, keys, values, w_gate, w_up, w_out):
    attended = window_attention(queries, keys, values)
    query_heads = queries.reshape(TOKENS, HEADS, HD).transpose(1, 0, 2)
    key_heads = keys.reshape(TOKENS, HEADS, HD).transpose(1, 0, 2)
    value_heads = values.reshape(TOKENS, HEADS, HD).transpose(1, 0, 2)

    def per_head(items):
        return fast_weight(items[0], items[1], items[2], items[3], items[4], items[5])
    learned = lax.map(per_head, (query_heads, key_heads, value_heads, w_gate, w_up, w_out))
    learned = learned.transpose(1, 0, 2).reshape(TOKENS, HEADS * HD)
    return (attended + learned).astype(jnp.bfloat16)
```

```python
import functools

import jax
import jax.numpy as jnp
from jax import lax
from jax.experimental import pallas as pl
from jax.experimental.pallas import tpu as pltpu
from jax.sharding import Mesh
from jax.sharding import PartitionSpec as P

HD = 512
WIN = 512
Y, Z, X = "ctx_0", "ctx_1", "ctx_2"
CTX = (Y, Z, X)
CTX_HEAD = CTX + ("head",)
MESH = pl.DeviceIdType.MESH
STEP = 0.02
EPS = 1e-06
F32, BF16 = jnp.float32, jnp.bfloat16


def dot(a, b, dims=((1,), (0,))):
    return lax.dot_general(a, b, (dims, ((), ())), preferred_element_type=F32)


class Copies:
    def __init__(self, send_sem, recv_sem):
        self.send_sem, self.recv_sem, self.count, self.all = send_sem, recv_sem, 0, []

    def start(self, src, dst, axis, index):
        copy = pltpu.make_async_remote_copy(
            src_ref=src,
            dst_ref=dst,
            send_sem=self.send_sem.at[self.count],
            recv_sem=self.recv_sem.at[self.count],
            device_id={axis: index},
            device_id_type=MESH,
        )
        self.count += 1
        copy.start()
        self.all.append(copy)
        return copy


def ring(axis):
    me = lax.axis_index(axis)
    return me, lax.rem(me + 1, 4), lax.rem(me + 3, 4), lax.rem(me + 2, 4)


def rows(base, index, size, part=0, parts=1):
    step = size // parts
    return pl.ds(pl.multiple_of(base + index * size + part * step, 16), step)


class RingReduce:
    def __init__(self, copies, axis, buf, c, opp, side):
        self.copies, self.axis, self.buf, self.c, self.opp, self.side = copies, axis, buf, c, opp, side
        me, right, left, far = ring(axis)
        half = c // 2
        s = lambda src, dst, to: copies.start(src, dst, axis, to)
        self.far_r = s(buf.at[:, rows(0, far, c, 0, 2), :], opp.at[0], right)
        self.far_l = s(buf.at[:, rows(0, far, c, 1, 2), :], opp.at[1], left)
        self.near_r = s(buf.at[:, rows(0, right, c, 1, 2), :], side.at[0, :, pl.ds(half, half), :], right)
        self.near_l = s(buf.at[:, rows(0, left, c, 0, 2), :], side.at[1, :, pl.ds(0, half), :], left)

    def middle(self):
        me, right, left, far = ring(self.axis)
        c, buf, half = self.c, self.buf, self.c // 2
        self.far_r.wait_recv()
        at = rows(0, right, c, 0, 2)
        buf[:, at, :] = (buf[:, at, :].astype(F32) + self.opp[0].astype(F32)).astype(BF16)
        self.last_r = self.copies.start(buf.at[:, at, :], self.side.at[0, :, pl.ds(0, half), :], self.axis, right)
        self.far_l.wait_recv()
        at = rows(0, left, c, 1, 2)
        buf[:, at, :] = (buf[:, at, :].astype(F32) + self.opp[1].astype(F32)).astype(BF16)
        self.last_l = self.copies.start(buf.at[:, at, :], self.side.at[1, :, pl.ds(half, half), :], self.axis, left)

    def end(self, out):
        me, right, left, far = ring(self.axis)
        for copy in (self.near_r, self.near_l, self.last_r, self.last_l):
            copy.wait_recv()
        own = self.buf[:, rows(0, me, self.c), :].astype(F32)
        out[...] = (own + self.side[0].astype(F32) + self.side[1].astype(F32)).astype(BF16)


class LineReduce:
    def __init__(self, copies, axis, buf, c, slots):
        me = lax.axis_index(axis)
        self.axis, self.buf, self.c, self.slots, self.sent = axis, buf, c, slots, []
        for d in (1, 2, 3):
            peer = lax.rem(me + d, 4)
            self.sent.append(copies.start(buf.at[:, rows(0, peer, c), :], slots.at[d - 1], axis, peer))

    def end(self):
        me = lax.axis_index(self.axis)
        total = self.buf[:, rows(0, me, self.c), :].astype(F32)
        for d in range(3):
            self.sent[d].wait_recv()
            total += self.slots[d].astype(F32)
        return total


class LineGather:
    def __init__(self, copies, axis, buf, base, c):
        me = lax.axis_index(axis)
        self.sent = []
        for d in (1, 2, 3):
            peer = lax.rem(me + d, 4)
            at = buf.at[:, rows(base, me, c), :]
            self.sent.append(copies.start(at, at, axis, peer))

    def end(self):
        for copy in self.sent:
            copy.wait_recv()


class RingGather:
    def __init__(self, copies, axis, buf, base, c):
        self.copies, self.axis, self.buf, self.base, self.c = copies, axis, buf, base, c
        me, right, left, far = ring(axis)
        low, high = (buf.at[:, rows(base, me, c, part, 2), :] for part in (0, 1))
        self.low_r = copies.start(low, low, axis, right)
        self.high_l = copies.start(high, high, axis, left)
        self.high_r = copies.start(high, high, axis, right)
        self.low_l = copies.start(low, low, axis, left)

    def middle(self):
        me, right, left, far = ring(self.axis)
        self.low_r.wait_recv()
        at = self.buf.at[:, rows(self.base, left, self.c, 0, 2), :]
        self.far_r = self.copies.start(at, at, self.axis, right)
        self.high_l.wait_recv()
        at = self.buf.at[:, rows(self.base, right, self.c, 1, 2), :]
        self.far_l = self.copies.start(at, at, self.axis, left)

    def end(self):
        for copy in (self.high_r, self.low_l, self.far_r, self.far_l):
            copy.wait_recv()


def fast_kernel(
    q_ref, k_ref, v_ref, wg_ref, wu_ref, wo_ref, out_ref,
    grad, opp1, side1, part2, opp2, side2, part3, slots, total, fresh, send_sem, recv_sem,
):
    barrier = pltpu.get_barrier_semaphore()
    for axis, offsets in ((X, (1, 3)), (Y, (1, 3)), (Z, (1, 2, 3))):
        for d in offsets:
            peer = lax.rem(lax.axis_index(axis) + d, 4)
            pl.semaphore_signal(barrier, inc=1, device_id={axis: peer}, device_id_type=MESH)

    copies = Copies(send_sem, recv_sem)
    order = ((X, Y), (Y, X))
    first = [None, None]
    for h in range(2):
        cols = pl.ds(h * HD, HD)
        k, v = k_ref[:, cols], v_ref[:, cols]
        a, b = dot(k, wg_ref[h]), dot(k, wu_ref[h])
        back = -dot(v, wo_ref[h], ((1,), (1,)))
        sig = jax.nn.sigmoid(a)
        act = a * sig
        hidden = (act * b).astype(BF16)
        da = (back * b * (sig * (1.0 + a * (1.0 - sig)))).astype(BF16)
        db = (back * act).astype(BF16)
        for m, g in enumerate(
            (dot(k, da, ((0,), (0,))), dot(k, db, ((0,), (0,))), -dot(hidden, v, ((0,), (0,))))
        ):
            grad[h, m, 0:HD, :] = g[:, 0:256].astype(BF16)
            grad[h, m, HD : 2 * HD, :] = g[:, 256:512].astype(BF16)
        if h == 0:
            pl.semaphore_wait(barrier, 7)
        first[h] = RingReduce(copies, order[h][0], grad.at[h], 256, opp1.at[h], side1.at[h])
    second, third, gather = [None, None], [None, None], [None, None]
    for h in range(2):
        first[h].middle()
    for h in range(2):
        first[h].end(part2.at[h])
        second[h] = RingReduce(copies, order[h][1], part2.at[h], 64, opp2.at[h], side2.at[h])
    for h in range(2):
        second[h].middle()
    for h in range(2):
        second[h].end(part3.at[h])
        third[h] = LineReduce(copies, Z, part3.at[h], 16, slots.at[h])
    bases = [lax.axis_index(order[h][0]) * 256 for h in range(2)]
    inner = [bases[h] + lax.axis_index(order[h][1]) * 64 for h in range(2)]
    for h in range(2):
        total[h, :, rows(inner[h], lax.axis_index(Z), 16), :] = third[h].end().astype(BF16)
        third[h] = LineGather(copies, Z, total.at[h], inner[h], 16)
    for h in range(2):
        third[h].end()
        gather[h] = RingGather(copies, order[h][1], total.at[h], bases[h], 64)
    for h in range(2):
        gather[h].middle()
    for h in range(2):
        gather[h].end()
        gather[h] = RingGather(copies, order[h][0], total.at[h], 0, 256)
    for h in range(2):
        gather[h].middle()
    for h in range(2):
        gather[h].end()
        for m, w_ref in enumerate((wg_ref, wu_ref, wo_ref)):
            g = total[h, m].astype(F32)
            scale = STEP * lax.rsqrt(jnp.sum(g * g) / (HD * HD) + EPS)
            for part in (0, 1):
                cols = pl.ds(part * 256, 256)
                piece = total[h, m, pl.ds(part * HD, HD), :].astype(F32)
                fresh[m, :, cols] = (w_ref[h, :, cols].astype(F32) - scale * piece).astype(BF16)
        cols = pl.ds(h * HD, HD)
        q = q_ref[:, cols]
        gate = dot(q, fresh[0])
        hid = (gate * jax.nn.sigmoid(gate) * dot(q, fresh[1])).astype(BF16)
        out_ref[:, cols] = dot(hid, fresh[2])
    for copy in copies.all:
        copy.wait_send()


def fast_weight(q, k, v, wg, wu, wo):
    vmem = pl.BlockSpec(memory_space=pltpu.VMEM)
    n_copies = 60
    return pl.pallas_call(
        fast_kernel,
        out_shape=jax.ShapeDtypeStruct((512, 1024), F32),
        in_specs=[vmem] * 6,
        out_specs=vmem,
        scratch_shapes=[
            pltpu.VMEM((2, 3, 1024, 256), BF16),
            pltpu.VMEM((2, 2, 3, 128, 256), BF16),
            pltpu.VMEM((2, 2, 3, 256, 256), BF16),
            pltpu.VMEM((2, 3, 256, 256), BF16),
            pltpu.VMEM((2, 2, 3, 32, 256), BF16),
            pltpu.VMEM((2, 2, 3, 64, 256), BF16),
            pltpu.VMEM((2, 3, 64, 256), BF16),
            pltpu.VMEM((2, 3, 3, 16, 256), BF16),
            pltpu.VMEM((2, 3, 1024, 256), BF16),
            pltpu.VMEM((3, HD, HD), BF16),
            pltpu.SemaphoreType.DMA((n_copies,)),
            pltpu.SemaphoreType.DMA((n_copies,)),
        ],
        compiler_params=pltpu.CompilerParams(
            collective_id=0, has_side_effects=True, vmem_limit_bytes=48 * 1024 * 1024
        ),
        cost_estimate=pl.CostEstimate(flops=40_000_000_000, bytes_accessed=10_000_000, transcendentals=0),
        name="fast_weight",
    )(q, k, v, wg, wu, wo)


def attend_kernel(q_ref, kp_ref, k_ref, kn_ref, vp_ref, v_ref, vn_ref, learned_ref, out_ref):
    block = (lax.axis_index(Y) * 4 + lax.axis_index(Z)) * 4 + lax.axis_index(X)
    has_before, has_after = block > 0, block < 63
    r = lax.broadcasted_iota(jnp.int32, (256, 256), 0)
    c = lax.broadcasted_iota(jnp.int32, (256, 256), 1)
    for h in range(2):
        cols = pl.ds(h * HD, HD)
        for t in range(2):
            top = pl.ds(t * 256, 256)
            q = q_ref[top, cols]
            before = pl.ds(t * 256, 512 - t * 256)
            after = pl.ds(0, 256 + t * 256)
            sb = dot(q, kp_ref[before, cols], ((1,), (1,))) * HD**-0.5
            so = dot(q, k_ref[:, cols], ((1,), (1,))) * HD**-0.5
            sa = dot(q, kn_ref[after, cols], ((1,), (1,))) * HD**-0.5
            edge_b = jnp.where((c >= r) & has_before, sb[:, :256], -1e30)
            edge_a = jnp.where((c <= r) & has_after, sa[:, t * 256 :], -1e30)
            if t == 0:
                pieces = [edge_b, jnp.where(has_before, sb[:, 256:], -1e30), so, edge_a]
            else:
                pieces = [edge_b, so, jnp.where(has_after, sa[:, :256], -1e30), edge_a]
            s = jnp.concatenate(pieces, axis=1)
            s = jnp.exp(s - jnp.max(s, axis=1, keepdims=True))
            p = (s / jnp.sum(s, axis=1, keepdims=True)).astype(BF16)
            nb = 512 - t * 256
            o = dot(p[:, :nb], vp_ref[before, cols]) + dot(p[:, nb : nb + 512], v_ref[:, cols])
            o += dot(p[:, nb + 512 :], vn_ref[after, cols])
            out_ref[top, cols] = (o + learned_ref[top, cols]).astype(BF16)


def attend(*args):
    vmem = pl.BlockSpec(memory_space=pltpu.VMEM)
    return pl.pallas_call(
        attend_kernel,
        out_shape=jax.ShapeDtypeStruct((512, 1024), BF16),
        in_specs=[vmem] * 8,
        out_specs=vmem,
        compiler_params=pltpu.CompilerParams(vmem_limit_bytes=48 * 1024 * 1024),
        cost_estimate=pl.CostEstimate(flops=3_000_000_000, bytes_accessed=10_000_000, transcendentals=1_300_000),
        name="attend",
    )(*args)


def neighbours(value):
    up = [(i, i + 1) for i in range(63)]
    down = [(i + 1, i) for i in range(63)]
    return lax.ppermute(value, CTX, up), lax.ppermute(value, CTX, down)


def per_device(queries, keys, values, w_gate, w_up, w_out):
    spread = lambda value: lax.all_to_all(value, "head", split_axis=1, concat_axis=0, tiled=True)
    k, v, q = spread(keys), spread(values), spread(queries)
    kp, kn = neighbours(k)
    vp, vn = neighbours(v)
    learned = fast_weight(q, k, v, w_gate, w_up, w_out)
    mixed = attend(q, kp, k, kn, vp, v, vn, learned)
    return lax.all_to_all(mixed, "head", split_axis=0, concat_axis=1, tiled=True)


def solution(mesh):
    split = Mesh(mesh.devices.reshape(4, 4, 4, 4), ("head", Y, Z, X))
    rows_spec, heads_spec = P(CTX_HEAD, None), P("head", None, None)
    return jax.shard_map(
        per_device,
        mesh=split,
        in_specs=(rows_spec,) * 3 + (heads_spec,) * 3,
        out_specs=rows_spec,
        check_vma=False,
    )
```

```python
import jax
import jax.numpy as jnp
from jax import lax
from jax.experimental import pallas as pl
from jax.experimental.pallas import tpu as pltpu
from jax.sharding import Mesh
from jax.sharding import PartitionSpec as P

HD = 512
WIN = 512
Y, Z, X = "ctx_0", "ctx_1", "ctx_2"
CTX = (Y, Z, X)
CTX_HEAD = CTX + ("head",)
MESH = pl.DeviceIdType.MESH
STEP = 0.02
EPS = 1e-06
F32, BF16 = jnp.float32, jnp.bfloat16


def dot(a, b, dims=((1,), (0,))):
    return lax.dot_general(a, b, (dims, ((), ())), preferred_element_type=F32)


class Copies:
    def __init__(self, send_sem, recv_sem):
        self.send_sem, self.recv_sem, self.count, self.all = send_sem, recv_sem, 0, []

    def make(self, src, dst, device):
        copy = pltpu.make_async_remote_copy(
            src_ref=src,
            dst_ref=dst,
            send_sem=self.send_sem.at[self.count],
            recv_sem=self.recv_sem.at[self.count],
            device_id=device,
            device_id_type=MESH,
        )
        self.count += 1
        self.all.append(copy)
        return copy

    def start(self, src, dst, device):
        copy = self.make(src, dst, device)
        copy.start()
        return copy


def ring(axis):
    me = lax.axis_index(axis)
    return me, lax.rem(me + 1, 4), lax.rem(me + 3, 4), lax.rem(me + 2, 4)


def rows(base, index, size, part=0, parts=1):
    step = size // parts
    return pl.ds(pl.multiple_of(base + index * size + part * step, 16), step)


def add_into(buf, at, other):
    buf[:, at, :] = (buf[:, at, :].astype(F32) + other.astype(F32)).astype(buf.dtype)


class RingReduce:
    def __init__(self, copies, axis, buf, c, opp, side):
        self.copies, self.axis, self.buf, self.c, self.opp, self.side = copies, axis, buf, c, opp, side
        me, right, left, far = ring(axis)
        half = c // 2
        r, l = {axis: right}, {axis: left}
        self.far_r = copies.start(buf.at[:, rows(0, far, c, 0, 2), :], opp.at[0], r)
        self.far_l = copies.start(buf.at[:, rows(0, far, c, 1, 2), :], opp.at[1], l)
        self.near_r = copies.start(buf.at[:, rows(0, right, c, 1, 2), :], side.at[0, :, pl.ds(half, half), :], r)
        self.near_l = copies.start(buf.at[:, rows(0, left, c, 0, 2), :], side.at[1, :, pl.ds(0, half), :], l)

    def middle(self):
        me, right, left, far = ring(self.axis)
        c, buf, half = self.c, self.buf, self.c // 2
        self.far_r.wait_recv()
        at = rows(0, right, c, 0, 2)
        add_into(buf, at, self.opp[0])
        self.last_r = self.copies.start(buf.at[:, at, :], self.side.at[0, :, pl.ds(0, half), :], {self.axis: right})
        self.far_l.wait_recv()
        at = rows(0, left, c, 1, 2)
        add_into(buf, at, self.opp[1])
        self.last_l = self.copies.start(buf.at[:, at, :], self.side.at[1, :, pl.ds(half, half), :], {self.axis: left})

    def end(self, out):
        me = lax.axis_index(self.axis)
        for copy in (self.near_r, self.near_l, self.last_r, self.last_l):
            copy.wait_recv()
        own = self.buf[:, rows(0, me, self.c), :].astype(F32)
        out[...] = own + self.side[0].astype(F32) + self.side[1].astype(F32)


class LineReduce:
    def __init__(self, copies, axis, buf, c, slots):
        me = lax.axis_index(axis)
        self.axis, self.buf, self.c, self.slots, self.sent = axis, buf, c, slots, []
        for d in (1, 2, 3):
            peer = lax.rem(me + d, 4)
            self.sent.append(copies.start(buf.at[:, rows(0, peer, c), :], slots.at[d - 1], {axis: peer}))

    def end(self):
        total = self.buf[:, rows(0, lax.axis_index(self.axis), self.c), :]
        for d in range(3):
            self.sent[d].wait_recv()
            total += self.slots[d]
        return total


class LineGather:
    def __init__(self, copies, axis, buf, base, c):
        me = lax.axis_index(axis)
        at = buf.at[:, rows(base, me, c), :]
        self.sent = [copies.start(at, at, {axis: lax.rem(me + d, 4)}) for d in (1, 2, 3)]

    def end(self):
        for copy in self.sent:
            copy.wait_recv()


class RingGather:
    def __init__(self, copies, axis, buf, base, c):
        self.copies, self.axis, self.buf, self.base, self.c = copies, axis, buf, base, c
        me, right, left, far = ring(axis)
        low, high = (buf.at[:, rows(base, me, c, part, 2), :] for part in (0, 1))
        self.low_r = copies.start(low, low, {axis: right})
        self.high_l = copies.start(high, high, {axis: left})
        self.high_r = copies.start(high, high, {axis: right})
        self.low_l = copies.start(low, low, {axis: left})

    def middle(self):
        me, right, left, far = ring(self.axis)
        self.low_r.wait_recv()
        at = self.buf.at[:, rows(self.base, left, self.c, 0, 2), :]
        self.far_r = self.copies.start(at, at, {self.axis: right})
        self.high_l.wait_recv()
        at = self.buf.at[:, rows(self.base, right, self.c, 1, 2), :]
        self.far_l = self.copies.start(at, at, {self.axis: left})

    def end(self):
        for copy in (self.high_r, self.low_l, self.far_r, self.far_l):
            copy.wait_recv()


class Group:
    def __init__(self, copies, g, bufs):
        self.copies, self.g = copies, g
        self.first, self.second = ((X, Y), (Y, X))[g % 2]
        self.b = {name: ref.at[g] for name, ref in bufs.items()}
        self.base = lax.axis_index(self.first) * 256
        self.inner = self.base + lax.axis_index(self.second) * 64

    def start(self):
        b = self.b
        self.now = RingReduce(self.copies, self.first, b["grad"], 256, b["opp1"], b["side1"])

    def middle(self):
        self.now.middle()

    def start2(self):
        b = self.b
        self.now.end(b["part2"])
        self.now = RingReduce(self.copies, self.second, b["part2"], 64, b["opp2"], b["side2"])

    def start3(self):
        b = self.b
        self.now.end(b["part3"])
        self.now = LineReduce(self.copies, Z, b["part3"], 16, b["slots"])

    def gather3(self):
        b = self.b
        b["total"][:, rows(self.inner, lax.axis_index(Z), 16), :] = self.now.end().astype(BF16)
        self.now = LineGather(self.copies, Z, b["total"], self.inner, 16)

    def gather2(self):
        self.now.end()
        self.now = RingGather(self.copies, self.second, self.b["total"], self.base, 64)

    def gather1(self):
        self.now.end()
        self.now = RingGather(self.copies, self.first, self.b["total"], 0, 256)

    def end(self):
        self.now.end()


def gradients(k, v, wg, wu, wo, grad, h):
    a, b = dot(k, wg), dot(k, wu)
    back = -dot(v, wo, ((1,), (1,)))
    sig = jax.nn.sigmoid(a)
    act = a * sig
    hidden = (act * b).astype(BF16)
    da = (back * b * (sig * (1.0 + a * (1.0 - sig)))).astype(BF16)
    db = (back * act).astype(BF16)
    pairs = ((k, da), (k, db), (hidden, v))
    for m, (left, right) in enumerate(pairs):
        g = dot(left, right, ((0,), (0,)))
        g = -g if m == 2 else g
        for part in range(4):
            at = pl.ds((part % 2) * HD, HD)
            grad[2 * h + part // 2, m, at, :] = g[:, part * 128 : part * 128 + 128].astype(BF16)


def update(total, weights, fresh, h):
    for m, w_ref in enumerate(weights):
        squares = 0.0
        for color in range(2):
            g = total[2 * h + color, m].astype(F32)
            squares += jnp.sum(g * g)
        scale = STEP * lax.rsqrt(squares / (HD * HD) + EPS)
        for part in range(4):
            cols = pl.ds(part * 128, 128)
            g = total[2 * h + part // 2, m, pl.ds((part % 2) * HD, HD), :].astype(F32)
            fresh[m, :, cols] = (w_ref[h, :, cols].astype(F32) - scale * g).astype(BF16)


def attention(q_ref, before, own, after, out, has_before, has_after):
    r = lax.broadcasted_iota(jnp.int32, (256, 256), 0)
    c = lax.broadcasted_iota(jnp.int32, (256, 256), 1)
    for t in range(2):
        top = pl.ds(t * 256, 256)
        q = q_ref[top, :]
        nb = 512 - t * 256
        late, early = pl.ds(t * 256, nb), pl.ds(0, 256 + t * 256)
        sb = dot(q, before[0, late, :], ((1,), (1,))) * HD**-0.5
        so = dot(q, own[0], ((1,), (1,))) * HD**-0.5
        sa = dot(q, after[0, early, :], ((1,), (1,))) * HD**-0.5
        pieces = [jnp.where((c >= r) & has_before, sb[:, :256], -1e30)]
        if t == 0:
            pieces += [jnp.where(has_before, sb[:, 256:], -1e30), so]
        else:
            pieces += [so, jnp.where(has_after, sa[:, :256], -1e30)]
        pieces.append(jnp.where((c <= r) & has_after, sa[:, t * 256 :], -1e30))
        s = jnp.concatenate(pieces, axis=1)
        s = jnp.exp(s - jnp.max(s, axis=1, keepdims=True))
        p = (s / jnp.sum(s, axis=1, keepdims=True)).astype(BF16)
        o = dot(p[:, :nb], before[1, late, :]) + dot(p[:, nb : nb + 512], own[1])
        out[top, :] = o + dot(p[:, nb + 512 :], after[1, early, :])


def shifted(delta):
    block = (lax.axis_index(Y) * 4 + lax.axis_index(Z)) * 4 + lax.axis_index(X)
    to = lax.rem(block + delta + 64, 64)
    return {Y: to // 16, Z: lax.rem(to // 4, 4), X: lax.rem(to, 4)}


def kernel(
    q_in, k_in, v_in, wg_in, wu_in, wo_in, out_ref,
    wg, wu, wo, q_all, kv, before, after, attended, mixed, fresh,
    grad, opp1, side1, part2, opp2, side2, part3, slots, total, send_sem, recv_sem, local_sem,
):
    g = lax.axis_index("head")
    hi, core = g // 2, lax.rem(g, 2)
    heads = ((1 - hi) * 2 + core, (1 - hi) * 2 + 1 - core, hi * 2 + 1 - core)
    barrier = pltpu.get_barrier_semaphore()
    partners = [{"head": p} for p in heads] + [shifted(1), shifted(-1)]
    for axis, offsets in ((X, (1, 3)), (Y, (1, 3)), (Z, (1, 2, 3))):
        partners += [{axis: lax.rem(lax.axis_index(axis) + d, 4)} for d in offsets]
    for p in partners:
        pl.semaphore_signal(barrier, inc=1, device_id=p, device_id_type=MESH)

    def cols(p, h):
        return pl.ds(pl.multiple_of(p * 1024 + h * HD, HD), HD)

    def place(ref, p):
        return ref.at[pl.ds(pl.multiple_of(p * 128, 128), 128), :]

    def half_rows(p):
        return pl.ds(pl.multiple_of(p * 256, 256), 256)

    local = []

    def stay(src, dst):
        copy = pltpu.make_async_copy(src, dst, local_sem.at[len(local)])
        copy.start()
        local.append(copy)

    for h in range(2):
        for i, ref in enumerate((k_in, v_in)):
            stay(ref.at[:, cols(g, h)], place(kv.at[i, h], g))
        stay(q_in.at[:, cols(g, h)], place(q_all.at[h], g))
    for src, dst in ((wg_in, wg), (wu_in, wu), (wo_in, wo)):
        stay(src, dst)

    copies = Copies(send_sem, recv_sem)
    pl.semaphore_wait(barrier, len(partners))
    sent = {}
    for h in range(2):
        for j, p in enumerate(heads):
            for i, ref in enumerate((k_in, v_in)):
                sent[h, j, i] = copies.start(ref.at[:, cols(p, h)], place(kv.at[i, h], g), {"head": p})
    for h in range(2):
        for j, p in enumerate(heads):
            sent[h, j, 2] = copies.start(q_in.at[:, cols(p, h)], place(q_all.at[h], g), {"head": p})

    def halo(src_index, at):
        found = []
        for dst, delta in ((before, 1), (after, -1)):
            found.append(copies.start(kv.at[src_index + (at, slice(None))], dst.at[src_index + (at, slice(None))], shifted(delta)))
        return found

    for copy in local:
        copy.wait()
    for h in range(2):
        for i in range(2):
            sent[h, 2, i].wait_recv()
    every = slice(None)
    halos = halo((every, every), half_rows(hi))

    bufs = dict(
        grad=grad, opp1=opp1, side1=side1, part2=part2, opp2=opp2, side2=side2, part3=part3, slots=slots, total=total
    )
    groups = [Group(copies, n, bufs) for n in range(4)]
    weights = (wg, wu, wo)

    def both(h, step):
        for group in groups[2 * h : 2 * h + 2]:
            getattr(group, step)()

    def head_in(h):
        for j in range(2):
            for i in range(2):
                sent[h, j, i].wait_recv()
        gradients(kv[0, h], kv[1, h], wg[h], wu[h], wo[h], grad, h)
        both(h, "start")

    has_before = sum(lax.axis_index(axis) for axis in CTX) > 0
    has_after = sum(lax.axis_index(axis) for axis in CTX) < 9

    def attend(h):
        attention(q_all.at[h], before.at[:, h], kv.at[:, h], after.at[:, h], attended.at[h], has_before, has_after)

    outs = {}

    def learn(h):
        update(total, weights, fresh, h)
        q = q_all[h]
        gate = dot(q, fresh[0])
        hid = (gate * jax.nn.sigmoid(gate) * dot(q, fresh[1])).astype(BF16)
        mixed[h] = (attended[h] + dot(hid, fresh[2])).astype(BF16)
        for j, p in enumerate(heads):
            outs[h, j] = copies.start(place(mixed.at[h], p), out_ref.at[:, cols(g, h)], {"head": p})
        out_ref[:, cols(g, h)] = mixed[h, pl.ds(pl.multiple_of(g * 128, 128), 128), :]

    head_in(0)
    both(0, "middle")
    both(0, "start2")
    both(0, "middle")
    halos += halo((every, 0), half_rows(1 - hi))
    both(0, "start3")
    head_in(1)
    both(0, "gather3")
    both(1, "middle")
    both(0, "gather2")
    both(1, "start2")
    both(0, "middle")
    both(1, "middle")
    halos += halo((every, 1), half_rows(1 - hi))
    both(0, "gather1")
    both(1, "start3")
    both(0, "middle")
    both(1, "gather3")
    both(1, "gather2")
    both(1, "middle")
    for copy in halos[:4]:
        copy.wait_recv()
    for h in range(2):
        for j in range(3):
            sent[h, j, 2].wait_recv()
    both(1, "gather1")
    attend(0)
    both(0, "end")
    both(1, "middle")
    learn(0)
    for copy in halos[4:]:
        copy.wait_recv()
    attend(1)
    both(1, "end")
    learn(1)
    for copy in outs.values():
        copy.wait_recv()
    for copy in copies.all:
        copy.wait_send()


def per_device(queries, keys, values, w_gate, w_up, w_out):
    anywhere = pl.BlockSpec(memory_space=pl.ANY)
    n_copies = 150
    wide, matrices = (2, HD, HD), (3, HD, HD)
    return pl.pallas_call(
        kernel,
        out_shape=jax.ShapeDtypeStruct((128, 4096), BF16),
        in_specs=[anywhere] * 6,
        out_specs=pl.BlockSpec(memory_space=pltpu.VMEM),
        scratch_shapes=[
            pltpu.VMEM(wide, BF16),
            pltpu.VMEM(wide, BF16),
            pltpu.VMEM(wide, BF16),
            pltpu.VMEM(wide, BF16),
            pltpu.VMEM((2,) + wide, BF16),
            pltpu.VMEM((2,) + wide, BF16),
            pltpu.VMEM((2,) + wide, BF16),
            pltpu.VMEM(wide, F32),
            pltpu.VMEM(wide, BF16),
            pltpu.VMEM(matrices, BF16),
            pltpu.VMEM((4, 3, 1024, 128), BF16),
            pltpu.VMEM((4, 2, 3, 128, 128), BF16),
            pltpu.VMEM((4, 2, 3, 256, 128), BF16),
            pltpu.VMEM((4, 3, 256, 128), F32),
            pltpu.VMEM((4, 2, 3, 32, 128), F32),
            pltpu.VMEM((4, 2, 3, 64, 128), F32),
            pltpu.VMEM((4, 3, 64, 128), F32),
            pltpu.VMEM((4, 3, 3, 16, 128), F32),
            pltpu.VMEM((4, 3, 1024, 128), BF16),
            pltpu.SemaphoreType.DMA((n_copies,)),
            pltpu.SemaphoreType.DMA((n_copies,)),
            pltpu.SemaphoreType.DMA((9,)),
        ],
        compiler_params=pltpu.CompilerParams(
            collective_id=0, has_side_effects=True, vmem_limit_bytes=56 * 1024 * 1024
        ),
        name="layer",
    )(queries, keys, values, w_gate, w_up, w_out)


def solution(mesh):
    split = Mesh(mesh.devices.reshape(4, 4, 4, 4), ("head", Y, Z, X))
    rows_spec, heads_spec = P(CTX_HEAD, None), P("head", None, None)
    return jax.shard_map(
        per_device,
        mesh=split,
        in_specs=(rows_spec,) * 3 + (heads_spec,) * 3,
        out_specs=rows_spec,
        check_vma=False,
    )
```

```python
import jax
import jax.numpy as jnp
from jax import lax
from jax.experimental import pallas as pl
from jax.experimental.pallas import tpu as pltpu
from jax.sharding import Mesh
from jax.sharding import PartitionSpec as P

HD = 512
WIN = 512
Y, Z, X = "ctx_0", "ctx_1", "ctx_2"
CTX = (Y, Z, X)
CTX_HEAD = CTX + ("head",)
MESH = pl.DeviceIdType.MESH
STEP = 0.02
EPS = 1e-06
F32, BF16 = jnp.float32, jnp.bfloat16


def dot(a, b, dims=((1,), (0,))):
    return lax.dot_general(a, b, (dims, ((), ())), preferred_element_type=F32)


class Copies:
    def __init__(self, send_sem, recv_sem):
        self.send_sem, self.recv_sem, self.count, self.all = send_sem, recv_sem, 0, []

    def make(self, src, dst, device):
        copy = pltpu.make_async_remote_copy(
            src_ref=src,
            dst_ref=dst,
            send_sem=self.send_sem.at[self.count],
            recv_sem=self.recv_sem.at[self.count],
            device_id=device,
            device_id_type=MESH,
        )
        self.count += 1
        return copy

    def start(self, src, dst, device):
        copy = self.make(src, dst, device)
        self.all.append(copy)
        copy.start()
        return copy


def ring(axis):
    me = lax.axis_index(axis)
    return me, lax.rem(me + 1, 4), lax.rem(me + 3, 4), lax.rem(me + 2, 4)


def rows(base, index, size, part=0, parts=1):
    step = size // parts
    return pl.ds(pl.multiple_of(base + index * size + part * step, 16), step)


def add_into(buf, at, other):
    buf[:, at, :] = (buf[:, at, :].astype(F32) + other.astype(F32)).astype(buf.dtype)


class RingReduce:
    def __init__(self, copies, axis, buf, c, opp, side):
        self.copies, self.axis, self.buf, self.c, self.opp, self.side = copies, axis, buf, c, opp, side
        me, right, left, far = ring(axis)
        half = c // 2
        r, l = {axis: right}, {axis: left}
        self.far_r = copies.start(buf.at[:, rows(0, far, c, 0, 2), :], opp.at[0], r)
        self.far_l = copies.start(buf.at[:, rows(0, far, c, 1, 2), :], opp.at[1], l)
        self.near_r = copies.start(buf.at[:, rows(0, right, c, 1, 2), :], side.at[0, :, pl.ds(half, half), :], r)
        self.near_l = copies.start(buf.at[:, rows(0, left, c, 0, 2), :], side.at[1, :, pl.ds(0, half), :], l)

    def middle(self):
        me, right, left, far = ring(self.axis)
        c, buf, half = self.c, self.buf, self.c // 2
        self.far_r.wait_recv()
        at = rows(0, right, c, 0, 2)
        add_into(buf, at, self.opp[0])
        self.last_r = self.copies.start(buf.at[:, at, :], self.side.at[0, :, pl.ds(0, half), :], {self.axis: right})
        self.far_l.wait_recv()
        at = rows(0, left, c, 1, 2)
        add_into(buf, at, self.opp[1])
        self.last_l = self.copies.start(buf.at[:, at, :], self.side.at[1, :, pl.ds(half, half), :], {self.axis: left})

    def end(self, out):
        me = lax.axis_index(self.axis)
        for copy in (self.near_r, self.near_l, self.last_r, self.last_l):
            copy.wait_recv()
        own = self.buf[:, rows(0, me, self.c), :].astype(F32)
        out[...] = own + self.side[0].astype(F32) + self.side[1].astype(F32)


class LineReduce:
    def __init__(self, copies, axis, buf, c, slots):
        me = lax.axis_index(axis)
        self.axis, self.buf, self.c, self.slots, self.sent = axis, buf, c, slots, []
        for d in (1, 2, 3):
            peer = lax.rem(me + d, 4)
            self.sent.append(copies.start(buf.at[:, rows(0, peer, c), :], slots.at[d - 1], {axis: peer}))

    def end(self):
        total = self.buf[:, rows(0, lax.axis_index(self.axis), self.c), :]
        for d in range(3):
            self.sent[d].wait_recv()
            total += self.slots[d]
        return total


class LineGather:
    def __init__(self, copies, axis, buf, base, c):
        me = lax.axis_index(axis)
        at = buf.at[:, rows(base, me, c), :]
        self.sent = [copies.start(at, at, {axis: lax.rem(me + d, 4)}) for d in (1, 2, 3)]

    def end(self):
        for copy in self.sent:
            copy.wait_recv()


class RingGather:
    def __init__(self, copies, axis, buf, base, c):
        self.copies, self.axis, self.buf, self.base, self.c = copies, axis, buf, base, c
        me, right, left, far = ring(axis)
        low, high = (buf.at[:, rows(base, me, c, part, 2), :] for part in (0, 1))
        self.low_r = copies.start(low, low, {axis: right})
        self.high_l = copies.start(high, high, {axis: left})
        self.high_r = copies.start(high, high, {axis: right})
        self.low_l = copies.start(low, low, {axis: left})

    def middle(self):
        me, right, left, far = ring(self.axis)
        self.low_r.wait_recv()
        at = self.buf.at[:, rows(self.base, left, self.c, 0, 2), :]
        self.far_r = self.copies.start(at, at, {self.axis: right})
        self.high_l.wait_recv()
        at = self.buf.at[:, rows(self.base, right, self.c, 1, 2), :]
        self.far_l = self.copies.start(at, at, {self.axis: left})

    def end(self):
        for copy in (self.high_r, self.low_l, self.far_r, self.far_l):
            copy.wait_recv()


class Group:
    def __init__(self, copies, g, bufs):
        self.copies, self.g = copies, g
        self.first, self.second = ((X, Y), (Y, X))[g % 2]
        self.b = {name: ref.at[g] for name, ref in bufs.items()}
        self.base = lax.axis_index(self.first) * 256
        self.inner = self.base + lax.axis_index(self.second) * 64

    def start(self):
        b = self.b
        self.now = RingReduce(self.copies, self.first, b["grad"], 256, b["opp1"], b["side1"])

    def middle(self):
        self.now.middle()

    def start2(self):
        b = self.b
        self.now.end(b["part2"])
        self.now = RingReduce(self.copies, self.second, b["part2"], 64, b["opp2"], b["side2"])

    def start3(self):
        b = self.b
        self.now.end(b["part3"])
        self.now = LineReduce(self.copies, Z, b["part3"], 16, b["slots"])

    def gather3(self):
        b = self.b
        b["total"][:, rows(self.inner, lax.axis_index(Z), 16), :] = self.now.end().astype(BF16)
        self.now = LineGather(self.copies, Z, b["total"], self.inner, 16)

    def gather2(self):
        self.now.end()
        self.now = RingGather(self.copies, self.second, self.b["total"], self.base, 64)

    def gather1(self):
        self.now.end()
        self.now = RingGather(self.copies, self.first, self.b["total"], 0, 256)

    def end(self):
        self.now.end()


def gradients(k, v, wg, wu, wo, grad, h):
    a, b = dot(k, wg), dot(k, wu)
    back = -dot(v, wo, ((1,), (1,)))
    sig = jax.nn.sigmoid(a)
    act = a * sig
    hidden = (act * b).astype(BF16)
    da = (back * b * (sig * (1.0 + a * (1.0 - sig)))).astype(BF16)
    db = (back * act).astype(BF16)
    pairs = ((k, da), (k, db), (hidden, v))
    for m, (left, right) in enumerate(pairs):
        g = dot(left, right, ((0,), (0,)))
        g = -g if m == 2 else g
        for part in range(4):
            at = pl.ds((part % 2) * HD, HD)
            grad[2 * h + part // 2, m, at, :] = g[:, part * 128 : part * 128 + 128].astype(BF16)


def update(total, weights, fresh, h):
    for m, w_ref in enumerate(weights):
        squares = 0.0
        for color in range(2):
            g = total[2 * h + color, m].astype(F32)
            squares += jnp.sum(g * g)
        scale = STEP * lax.rsqrt(squares / (HD * HD) + EPS)
        for part in range(4):
            cols = pl.ds(part * 128, 128)
            g = total[2 * h + part // 2, m, pl.ds((part % 2) * HD, HD), :].astype(F32)
            fresh[m, :, cols] = (w_ref[h, :, cols].astype(F32) - scale * g).astype(BF16)


def attention(q_ref, before, own, after, out, has_before, has_after):
    r = lax.broadcasted_iota(jnp.int32, (256, 256), 0)
    c = lax.broadcasted_iota(jnp.int32, (256, 256), 1)
    for t in range(2):
        top = pl.ds(t * 256, 256)
        q = q_ref[top, :]
        nb = 512 - t * 256
        late, early = pl.ds(t * 256, nb), pl.ds(0, 256 + t * 256)
        sb = dot(q, before[0, late, :], ((1,), (1,))) * HD**-0.5
        so = dot(q, own[0], ((1,), (1,))) * HD**-0.5
        sa = dot(q, after[0, early, :], ((1,), (1,))) * HD**-0.5
        pieces = [jnp.where((c >= r) & has_before, sb[:, :256], -1e30)]
        if t == 0:
            pieces += [jnp.where(has_before, sb[:, 256:], -1e30), so]
        else:
            pieces += [so, jnp.where(has_after, sa[:, :256], -1e30)]
        pieces.append(jnp.where((c <= r) & has_after, sa[:, t * 256 :], -1e30))
        s = jnp.concatenate(pieces, axis=1)
        s = jnp.exp(s - jnp.max(s, axis=1, keepdims=True))
        p = (s / jnp.sum(s, axis=1, keepdims=True)).astype(BF16)
        o = dot(p[:, :nb], before[1, late, :]) + dot(p[:, nb : nb + 512], own[1])
        out[top, :] = o + dot(p[:, nb + 512 :], after[1, early, :])


def row(delta, x):
    to = lax.rem(lax.axis_index(Y) * 4 + lax.axis_index(Z) + delta + 16, 16)
    return {Y: to // 4, Z: lax.rem(to, 4), X: jnp.int32(x)}


class Halo:
    def __init__(self, copies, kv, dst, relay, delta, hi):
        x = lax.axis_index(X)
        self.source, self.last = (3, 0) if delta == 1 else (0, 3)
        self.x, self.copies = x, copies
        self.is_source, self.is_last = x == self.source, x == self.last
        nearby = {X: lax.rem(x + delta + 4, 4)}
        every = slice(None)
        own = pl.ds(pl.multiple_of(hi * 256, 256), 256)
        other = pl.ds(pl.multiple_of((1 - hi) * 256, 256), 256)
        self.early = copies.make(kv.at[:, :, own, :], dst.at[:, :, own, :], nearby)
        self.cross = [copies.make(kv.at[:, h, other, :], dst.at[:, h, other, :], nearby) for h in range(2)]
        self.leg1, self.leg2 = {}, {}
        for c in range(4):
            piece = kv.at[c % 2, c // 2]
            if c != self.source:
                self.leg1[c] = copies.make(piece, relay, {X: jnp.int32(c)})
                piece = relay
            self.leg2[c] = copies.make(piece, dst.at[c % 2, c // 2], row(delta, self.last))

    def send_early(self):
        pl.when(jnp.logical_not(self.is_source))(self.early.start)

    def send(self, h):
        pl.when(jnp.logical_not(self.is_source))(self.cross[h].start)

        @pl.when(self.is_source)
        def _():
            for c in (2 * h, 2 * h + 1):
                (self.leg2 if c == self.source else self.leg1)[c].start()

    def relay(self, h):
        for c in (2 * h, 2 * h + 1):
            if c != self.source:

                @pl.when(self.x == c)
                def _():
                    self.leg1[c].wait_recv()
                    self.leg2[c].start()

    def receive(self, h):
        @pl.when(self.is_last)
        def _():
            for c in (2 * h, 2 * h + 1):
                self.leg2[c].wait_recv()

        @pl.when(jnp.logical_not(self.is_last))
        def _():
            if h == 0:
                self.early.wait_recv()
            self.cross[h].wait_recv()

    def finish(self):
        @pl.when(jnp.logical_not(self.is_source))
        def _():
            self.early.wait_send()
            for h in range(2):
                self.cross[h].wait_send()

        @pl.when(self.is_source)
        def _():
            for copy in self.leg1.values():
                copy.wait_send()

        for c in range(4):
            pl.when(self.x == c)(self.leg2[c].wait_send)


def kernel(
    q_in, k_in, v_in, wg_in, wu_in, wo_in, out_ref,
    wg, wu, wo, q_all, kv, before, after, relays, attended, mixed, fresh,
    grad, opp1, side1, part2, opp2, side2, part3, slots, total, send_sem, recv_sem, local_sem,
):
    g = lax.axis_index("head")
    hi, core = g // 2, lax.rem(g, 2)
    heads = ((1 - hi) * 2 + core, (1 - hi) * 2 + 1 - core, hi * 2 + 1 - core)
    barrier = pltpu.get_barrier_semaphore()
    partners = [{"head": p} for p in heads]
    for axis, offsets in ((X, (1, 2, 3)), (Y, (1, 3)), (Z, (1, 2, 3))):
        partners += [{axis: lax.rem(lax.axis_index(axis) + d, 4)} for d in offsets]
    for p in partners:
        pl.semaphore_signal(barrier, inc=1, device_id=p, device_id_type=MESH)
    for x, delta in ((0, -1), (3, 1)):

        @pl.when(lax.axis_index(X) == x)
        def _():
            for c in range(4):
                pl.semaphore_signal(barrier, inc=1, device_id=row(delta, c), device_id_type=MESH)

    def cols(p, h):
        return pl.ds(pl.multiple_of(p * 1024 + h * HD, HD), HD)

    def place(ref, p):
        return ref.at[pl.ds(pl.multiple_of(p * 128, 128), 128), :]

    local = []

    def stay(src, dst):
        copy = pltpu.make_async_copy(src, dst, local_sem.at[len(local)])
        copy.start()
        local.append(copy)

    for h in range(2):
        for i, ref in enumerate((k_in, v_in)):
            stay(ref.at[:, cols(g, h)], place(kv.at[i, h], g))
        stay(q_in.at[:, cols(g, h)], place(q_all.at[h], g))
    for src, dst in ((wg_in, wg), (wu_in, wu), (wo_in, wo)):
        stay(src, dst)

    copies = Copies(send_sem, recv_sem)
    pl.semaphore_wait(barrier, len(partners) + 2)
    sent = {}
    for h in range(2):
        for j, p in enumerate(heads):
            for i, ref in enumerate((k_in, v_in)):
                sent[h, j, i] = copies.start(ref.at[:, cols(p, h)], place(kv.at[i, h], g), {"head": p})

    def send_queries(h):
        for j, p in enumerate(heads):
            sent[h, j, 2] = copies.start(q_in.at[:, cols(p, h)], place(q_all.at[h], g), {"head": p})

    halos = [Halo(copies, kv, dst, relays.at[j], delta, hi) for j, (dst, delta) in enumerate(((before, 1), (after, -1)))]

    def halo(step, *args):
        for h in halos:
            getattr(h, step)(*args)

    for copy in local:
        copy.wait()
    for h in range(2):
        for i in range(2):
            sent[h, 2, i].wait_recv()
    halo("send_early")

    bufs = dict(
        grad=grad, opp1=opp1, side1=side1, part2=part2, opp2=opp2, side2=side2, part3=part3, slots=slots, total=total
    )
    groups = [Group(copies, n, bufs) for n in range(4)]
    weights = (wg, wu, wo)

    def both(h, step):
        for group in groups[2 * h : 2 * h + 2]:
            getattr(group, step)()

    def head_in(h):
        for j in range(2):
            for i in range(2):
                sent[h, j, i].wait_recv()
        gradients(kv[0, h], kv[1, h], wg[h], wu[h], wo[h], grad, h)
        both(h, "start")

    has_before = sum(lax.axis_index(axis) for axis in CTX) > 0
    has_after = sum(lax.axis_index(axis) for axis in CTX) < 9

    def attend(h):
        halo("receive", h)
        for j in range(3):
            sent[h, j, 2].wait_recv()
        attention(q_all.at[h], before.at[:, h], kv.at[:, h], after.at[:, h], attended.at[h], has_before, has_after)

    outs = {}

    def learn(h):
        update(total, weights, fresh, h)
        q = q_all[h]
        gate = dot(q, fresh[0])
        hid = (gate * jax.nn.sigmoid(gate) * dot(q, fresh[1])).astype(BF16)
        mixed[h] = (attended[h] + dot(hid, fresh[2])).astype(BF16)
        for j, p in enumerate(heads):
            outs[h, j] = copies.start(place(mixed.at[h], p), out_ref.at[:, cols(g, h)], {"head": p})
        out_ref[:, cols(g, h)] = mixed[h, pl.ds(pl.multiple_of(g * 128, 128), 128), :]

    head_in(0)
    both(0, "middle")
    both(0, "start2")
    halo("send", 0)
    both(0, "middle")
    both(0, "start3")
    send_queries(0)
    head_in(1)
    halo("relay", 0)
    both(0, "gather3")
    both(1, "middle")
    send_queries(1)
    both(0, "gather2")
    both(1, "start2")
    halo("send", 1)
    both(0, "middle")
    both(1, "middle")
    both(0, "gather1")
    both(1, "start3")
    halo("relay", 1)
    both(0, "middle")
    both(1, "gather3")
    attend(0)
    both(1, "gather2")
    both(0, "end")
    learn(0)
    both(1, "middle")
    both(1, "gather1")
    attend(1)
    both(1, "middle")
    both(1, "end")
    learn(1)
    for copy in outs.values():
        copy.wait_recv()
    for copy in copies.all:
        copy.wait_send()
    halo("finish")


def per_device(queries, keys, values, w_gate, w_up, w_out):
    anywhere = pl.BlockSpec(memory_space=pl.ANY)
    n_copies = 164
    wide, matrices = (2, HD, HD), (3, HD, HD)
    return pl.pallas_call(
        kernel,
        out_shape=jax.ShapeDtypeStruct((128, 4096), BF16),
        in_specs=[anywhere] * 6,
        out_specs=pl.BlockSpec(memory_space=pltpu.VMEM),
        scratch_shapes=[
            pltpu.VMEM(wide, BF16),
            pltpu.VMEM(wide, BF16),
            pltpu.VMEM(wide, BF16),
            pltpu.VMEM(wide, BF16),
            pltpu.VMEM((2,) + wide, BF16),
            pltpu.VMEM((2,) + wide, BF16),
            pltpu.VMEM((2,) + wide, BF16),
            pltpu.VMEM(wide, BF16),
            pltpu.VMEM(wide, F32),
            pltpu.VMEM(wide, BF16),
            pltpu.VMEM(matrices, BF16),
            pltpu.VMEM((4, 3, 1024, 128), BF16),
            pltpu.VMEM((4, 2, 3, 128, 128), BF16),
            pltpu.VMEM((4, 2, 3, 256, 128), BF16),
            pltpu.VMEM((4, 3, 256, 128), F32),
            pltpu.VMEM((4, 2, 3, 32, 128), F32),
            pltpu.VMEM((4, 2, 3, 64, 128), F32),
            pltpu.VMEM((4, 3, 64, 128), F32),
            pltpu.VMEM((4, 3, 3, 16, 128), F32),
            pltpu.VMEM((4, 3, 1024, 128), BF16),
            pltpu.SemaphoreType.DMA((n_copies,)),
            pltpu.SemaphoreType.DMA((n_copies,)),
            pltpu.SemaphoreType.DMA((9,)),
        ],
        compiler_params=pltpu.CompilerParams(
            collective_id=0, has_side_effects=True, vmem_limit_bytes=56 * 1024 * 1024
        ),
        name="layer",
    )(queries, keys, values, w_gate, w_up, w_out)


def solution(mesh):
    split = Mesh(mesh.devices.reshape(4, 4, 4, 4), ("head", Y, Z, X))
    rows_spec, heads_spec = P(CTX_HEAD, None), P("head", None, None)
    return jax.shard_map(
        per_device,
        mesh=split,
        in_specs=(rows_spec,) * 3 + (heads_spec,) * 3,
        out_specs=rows_spec,
        check_vma=False,
    )
```

```python
import jax
import jax.numpy as jnp
from jax import lax
from jax.experimental import pallas as pl
from jax.experimental.pallas import tpu as pltpu
from jax.sharding import Mesh
from jax.sharding import PartitionSpec as P

HD = 512
WIN = 512
Y, Z, X = "ctx_0", "ctx_1", "ctx_2"
CTX = (Y, Z, X)
CTX_HEAD = CTX + ("head",)
MESH = pl.DeviceIdType.MESH
STEP = 0.02
EPS = 1e-06
F32, BF16 = jnp.float32, jnp.bfloat16


def dot(a, b, dims=((1,), (0,))):
    return lax.dot_general(a, b, (dims, ((), ())), preferred_element_type=F32)


class Copies:
    def __init__(self, send_sem, recv_sem):
        self.send_sem, self.recv_sem, self.count, self.all = send_sem, recv_sem, 0, []

    def make(self, src, dst, device):
        copy = pltpu.make_async_remote_copy(
            src_ref=src,
            dst_ref=dst,
            send_sem=self.send_sem.at[self.count],
            recv_sem=self.recv_sem.at[self.count],
            device_id=device,
            device_id_type=MESH,
        )
        self.count += 1
        return copy

    def start(self, src, dst, device):
        copy = self.make(src, dst, device)
        self.all.append(copy)
        copy.start()
        return copy


def ring(axis):
    me = lax.axis_index(axis)
    return me, lax.rem(me + 1, 4), lax.rem(me + 3, 4), lax.rem(me + 2, 4)


def rows(base, index, size, part=0, parts=1):
    step = size // parts
    return pl.ds(pl.multiple_of(base + index * size + part * step, 16), step)


def add_into(buf, at, other):
    buf[:, at, :] = (buf[:, at, :].astype(F32) + other.astype(F32)).astype(buf.dtype)


class RingReduce:
    def __init__(self, copies, axis, buf, c, opp, side):
        self.copies, self.axis, self.buf, self.c, self.opp, self.side = copies, axis, buf, c, opp, side
        me, right, left, far = ring(axis)
        half = c // 2
        r, l = {axis: right}, {axis: left}
        self.far_r = copies.start(buf.at[:, rows(0, far, c, 0, 2), :], opp.at[0], r)
        self.far_l = copies.start(buf.at[:, rows(0, far, c, 1, 2), :], opp.at[1], l)
        self.near_r = copies.start(buf.at[:, rows(0, right, c, 1, 2), :], side.at[0, :, pl.ds(half, half), :], r)
        self.near_l = copies.start(buf.at[:, rows(0, left, c, 0, 2), :], side.at[1, :, pl.ds(0, half), :], l)

    def middle(self):
        me, right, left, far = ring(self.axis)
        c, buf, half = self.c, self.buf, self.c // 2
        self.far_r.wait_recv()
        at = rows(0, right, c, 0, 2)
        add_into(buf, at, self.opp[0])
        self.last_r = self.copies.start(buf.at[:, at, :], self.side.at[0, :, pl.ds(0, half), :], {self.axis: right})
        self.far_l.wait_recv()
        at = rows(0, left, c, 1, 2)
        add_into(buf, at, self.opp[1])
        self.last_l = self.copies.start(buf.at[:, at, :], self.side.at[1, :, pl.ds(half, half), :], {self.axis: left})

    def end(self, out):
        me = lax.axis_index(self.axis)
        for copy in (self.near_r, self.near_l, self.last_r, self.last_l):
            copy.wait_recv()
        own = self.buf[:, rows(0, me, self.c), :].astype(F32)
        out[...] = own + self.side[0].astype(F32) + self.side[1].astype(F32)


class LineReduce:
    def __init__(self, copies, axis, buf, c, slots):
        me = lax.axis_index(axis)
        self.axis, self.buf, self.c, self.slots, self.sent = axis, buf, c, slots, []
        for d in (1, 2, 3):
            peer = lax.rem(me + d, 4)
            self.sent.append(copies.start(buf.at[:, rows(0, peer, c), :], slots.at[d - 1], {axis: peer}))

    def end(self):
        total = self.buf[:, rows(0, lax.axis_index(self.axis), self.c), :]
        for d in range(3):
            self.sent[d].wait_recv()
            total += self.slots[d]
        return total


class LineGather:
    def __init__(self, copies, axis, buf, base, c):
        me = lax.axis_index(axis)
        at = buf.at[:, rows(base, me, c), :]
        self.sent = [copies.start(at, at, {axis: lax.rem(me + d, 4)}) for d in (1, 2, 3)]

    def end(self):
        for copy in self.sent:
            copy.wait_recv()


class RingGather:
    def __init__(self, copies, axis, buf, base, c):
        self.copies, self.axis, self.buf, self.base, self.c = copies, axis, buf, base, c
        me, right, left, far = ring(axis)
        low, high = (buf.at[:, rows(base, me, c, part, 2), :] for part in (0, 1))
        self.low_r = copies.start(low, low, {axis: right})
        self.high_l = copies.start(high, high, {axis: left})
        self.high_r = copies.start(high, high, {axis: right})
        self.low_l = copies.start(low, low, {axis: left})

    def middle(self):
        me, right, left, far = ring(self.axis)
        self.low_r.wait_recv()
        at = self.buf.at[:, rows(self.base, left, self.c, 0, 2), :]
        self.far_r = self.copies.start(at, at, {self.axis: right})
        self.high_l.wait_recv()
        at = self.buf.at[:, rows(self.base, right, self.c, 1, 2), :]
        self.far_l = self.copies.start(at, at, {self.axis: left})

    def end(self):
        for copy in (self.high_r, self.low_l, self.far_r, self.far_l):
            copy.wait_recv()


class Group:
    def __init__(self, copies, g, bufs):
        self.copies, self.g = copies, g
        self.first, self.second = (Y, X)
        self.b = {name: ref.at[g] for name, ref in bufs.items()}
        self.base = lax.axis_index(self.first) * 256
        self.inner = self.base + lax.axis_index(self.second) * 64

    def start(self):
        b = self.b
        self.now = RingReduce(self.copies, self.first, b["grad"], 256, b["opp1"], b["side1"])

    def middle(self):
        self.now.middle()

    def start2(self):
        b = self.b
        self.now.end(b["part2"])
        self.now = RingReduce(self.copies, self.second, b["part2"], 64, b["opp2"], b["side2"])

    def start3(self):
        b = self.b
        self.now.end(b["part3"])
        self.now = LineReduce(self.copies, Z, b["part3"], 16, b["slots"])

    def gather3(self):
        b = self.b
        b["total"][:, rows(self.inner, lax.axis_index(Z), 16), :] = self.now.end().astype(BF16)
        self.now = LineGather(self.copies, Z, b["total"], self.inner, 16)

    def gather2(self):
        self.now.end()
        self.now = RingGather(self.copies, self.second, self.b["total"], self.base, 64)

    def gather1(self):
        self.now.end()
        self.now = RingGather(self.copies, self.first, self.b["total"], 0, 256)

    def end(self):
        self.now.end()


def gradients(k, v, wg, wu, wo, grad, h):
    a, b = dot(k, wg), dot(k, wu)
    back = -dot(v, wo, ((1,), (1,)))
    sig = jax.nn.sigmoid(a)
    act = a * sig
    hidden = (act * b).astype(BF16)
    da = (back * b * (sig * (1.0 + a * (1.0 - sig)))).astype(BF16)
    db = (back * act).astype(BF16)
    pairs = ((k, da), (k, db), (hidden, v))
    for m, (left, right) in enumerate(pairs):
        g = dot(left, right, ((0,), (0,)))
        g = -g if m == 2 else g
        for part in range(4):
            at = pl.ds((part % 2) * HD, HD)
            grad[2 * h + part // 2, m, at, :] = g[:, part * 128 : part * 128 + 128].astype(BF16)


def update(total, weights, fresh, h):
    for m, w_ref in enumerate(weights):
        squares = 0.0
        for color in range(2):
            g = total[2 * h + color, m].astype(F32)
            squares += jnp.sum(g * g)
        scale = STEP * lax.rsqrt(squares / (HD * HD) + EPS)
        for part in range(4):
            cols = pl.ds(part * 128, 128)
            g = total[2 * h + part // 2, m, pl.ds((part % 2) * HD, HD), :].astype(F32)
            fresh[m, :, cols] = (w_ref[h, :, cols].astype(F32) - scale * g).astype(BF16)


def attention(q_ref, before, own, after, out, has_before, has_after):
    r = lax.broadcasted_iota(jnp.int32, (256, 256), 0)
    c = lax.broadcasted_iota(jnp.int32, (256, 256), 1)
    for t in range(2):
        top = pl.ds(t * 256, 256)
        q = q_ref[top, :]
        nb = 512 - t * 256
        late, early = pl.ds(t * 256, nb), pl.ds(0, 256 + t * 256)
        sb = dot(q, before[0, late, :], ((1,), (1,))) * HD**-0.5
        so = dot(q, own[0], ((1,), (1,))) * HD**-0.5
        sa = dot(q, after[0, early, :], ((1,), (1,))) * HD**-0.5
        pieces = [jnp.where((c >= r) & has_before, sb[:, :256], -1e30)]
        if t == 0:
            pieces += [jnp.where(has_before, sb[:, 256:], -1e30), so]
        else:
            pieces += [so, jnp.where(has_after, sa[:, :256], -1e30)]
        pieces.append(jnp.where((c <= r) & has_after, sa[:, t * 256 :], -1e30))
        s = jnp.concatenate(pieces, axis=1)
        s = jnp.exp(s - jnp.max(s, axis=1, keepdims=True))
        p = (s / jnp.sum(s, axis=1, keepdims=True)).astype(BF16)
        o = dot(p[:, :nb], before[1, late, :]) + dot(p[:, nb : nb + 512], own[1])
        out[top, :] = o + dot(p[:, nb + 512 :], after[1, early, :])


class Halo:
    def __init__(self, copies, kv, dst, relays, delta, hi):
        x, y, z = (lax.axis_index(axis) for axis in (X, Y, Z))
        self.source, self.last = (3, 0) if delta == 1 else (0, 3)
        self.x = x
        self.is_source, self.is_last = x == self.source, x == self.last
        self.leaves_y, self.enters_y = z == self.source, z == self.last
        ahead = lax.rem(z + delta + 4, 4)
        onward = lax.select(self.enters_y, lax.rem(y + delta + 4, 4), y)
        nearby = {X: lax.rem(x + delta + 4, 4)}
        every = slice(None)
        own = pl.ds(pl.multiple_of(hi * 256, 256), 256)
        other = pl.ds(pl.multiple_of((1 - hi) * 256, 256), 256)
        self.early = copies.make(kv.at[:, :, own, :], dst.at[:, :, own, :], nearby)
        self.cross = [copies.make(kv.at[:, h, other, :], dst.at[:, h, other, :], nearby) for h in range(2)]
        self.leg1, self.leg2, self.leg3 = {}, {}, {}
        for c in range(4):
            piece, end = kv.at[c % 2, c // 2], dst.at[c % 2, c // 2]
            if c != self.source:
                self.leg1[c] = copies.make(piece, relays.at[0], {X: jnp.int32(c)})
                piece = relays.at[0]
            self.leg2[c] = copies.make(piece, relays.at[1], {Z: ahead})
            if c == self.last:
                self.short = copies.make(piece, end, {Z: ahead})
            self.leg3[c] = copies.make(relays.at[1], end, {Y: onward, X: jnp.int32(self.last)})

    def send_early(self):
        pl.when(jnp.logical_not(self.is_source))(self.early.start)

    def send(self, h):
        pl.when(jnp.logical_not(self.is_source))(self.cross[h].start)

        @pl.when(self.is_source)
        def _():
            for c in (2 * h, 2 * h + 1):
                if c != self.source:
                    self.leg1[c].start()

    def second(self, c, step):
        if c == self.last:
            pl.when((self.x == c) & self.leaves_y)(lambda: getattr(self.leg2[c], step)())
            pl.when((self.x == c) & jnp.logical_not(self.leaves_y))(lambda: getattr(self.short, step)())
        else:
            pl.when(self.x == c)(lambda: getattr(self.leg2[c], step)())

    def third(self, c):
        return (self.x == c) & self.enters_y if c == self.last else self.x == c

    def relay(self, h):
        for c in (2 * h, 2 * h + 1):
            if c != self.source:
                pl.when(self.x == c)(self.leg1[c].wait_recv)
            self.second(c, "start")

    def forward(self, c, condition):
        @pl.when((self.x == c) & condition)
        def _():
            self.leg2[c].wait_recv()
            self.leg3[c].start()

    def relay2(self, h):
        for c in (2 * h, 2 * h + 1):
            if c != self.last:
                self.forward(c, jnp.logical_not(self.enters_y))

    def relay2_y(self):
        for c in range(4):
            self.forward(c, self.enters_y)

    def receive(self, h):
        for c in (2 * h, 2 * h + 1):
            if c == self.last:
                pl.when(self.is_last & self.enters_y)(self.leg3[c].wait_recv)
                pl.when(self.is_last & jnp.logical_not(self.enters_y))(self.short.wait_recv)
            else:
                pl.when(self.is_last)(self.leg3[c].wait_recv)

        @pl.when(jnp.logical_not(self.is_last))
        def _():
            if h == 0:
                self.early.wait_recv()
            self.cross[h].wait_recv()

    def finish(self):
        @pl.when(jnp.logical_not(self.is_source))
        def _():
            self.early.wait_send()
            for h in range(2):
                self.cross[h].wait_send()

        @pl.when(self.is_source)
        def _():
            for copy in self.leg1.values():
                copy.wait_send()

        for c in range(4):
            self.second(c, "wait_send")
            pl.when(self.third(c))(self.leg3[c].wait_send)


def kernel(
    q_in, k_in, v_in, wg_in, wu_in, wo_in, out_ref,
    wg, wu, wo, q_all, kv, before, after, relays, attended, mixed, fresh,
    grad, opp1, side1, part2, opp2, side2, part3, slots, total, send_sem, recv_sem, local_sem,
):
    g = lax.axis_index("head")
    hi, core = g // 2, lax.rem(g, 2)
    heads = ((1 - hi) * 2 + core, (1 - hi) * 2 + 1 - core, hi * 2 + 1 - core)
    barrier = pltpu.get_barrier_semaphore()
    partners = [{"head": p} for p in heads]
    for axis, offsets in ((X, (1, 2, 3)), (Y, (1, 3)), (Z, (1, 2, 3))):
        partners += [{axis: lax.rem(lax.axis_index(axis) + d, 4)} for d in offsets]
    for p in partners:
        pl.semaphore_signal(barrier, inc=1, device_id=p, device_id_type=MESH)
    for corner, step in ((0, 3), (3, 1)):
        above = {Y: lax.rem(lax.axis_index(Y) + step, 4)}

        @pl.when(lax.axis_index(X) == corner)
        def _():
            for c in range(4):
                pl.semaphore_signal(barrier, inc=1, device_id=above | {X: jnp.int32(c)}, device_id_type=MESH)

    def cols(p, h):
        return pl.ds(pl.multiple_of(p * 1024 + h * HD, HD), HD)

    def place(ref, p):
        return ref.at[pl.ds(pl.multiple_of(p * 128, 128), 128), :]

    local = []

    def stay(src, dst):
        copy = pltpu.make_async_copy(src, dst, local_sem.at[len(local)])
        copy.start()
        local.append(copy)

    for h in range(2):
        for i, ref in enumerate((k_in, v_in)):
            stay(ref.at[:, cols(g, h)], place(kv.at[i, h], g))
        stay(q_in.at[:, cols(g, h)], place(q_all.at[h], g))
    for src, dst in ((wg_in, wg), (wu_in, wu), (wo_in, wo)):
        stay(src, dst)

    copies = Copies(send_sem, recv_sem)
    pl.semaphore_wait(barrier, len(partners) + 2)
    sent = {}

    def send_pairs(h, js):
        for j in js:
            for i, ref in enumerate((k_in, v_in)):
                sent[h, j, i] = copies.start(ref.at[:, cols(heads[j], h)], place(kv.at[i, h], g), {"head": heads[j]})

    send_pairs(0, (0, 1, 2))
    send_pairs(1, (2,))

    def send_queries(h):
        for j, p in enumerate(heads):
            sent[h, j, 2] = copies.start(q_in.at[:, cols(p, h)], place(q_all.at[h], g), {"head": p})

    halos = [Halo(copies, kv, dst, relays.at[j], delta, hi) for j, (dst, delta) in enumerate(((before, 1), (after, -1)))]

    def halo(step, *args):
        for h in halos:
            getattr(h, step)(*args)

    for copy in local:
        copy.wait()
    for h in range(2):
        for i in range(2):
            sent[h, 2, i].wait_recv()
    halo("send_early")

    bufs = dict(
        grad=grad, opp1=opp1, side1=side1, part2=part2, opp2=opp2, side2=side2, part3=part3, slots=slots, total=total
    )
    groups = [Group(copies, n, bufs) for n in range(4)]
    weights = (wg, wu, wo)

    def both(h, step):
        for group in groups[2 * h : 2 * h + 2]:
            getattr(group, step)()

    def head_in(h):
        for j in range(2):
            for i in range(2):
                sent[h, j, i].wait_recv()
        if h == 0:
            send_pairs(1, (0, 1))
            halo("send", 0)
        else:
            send_queries(0)
            send_queries(1)
        gradients(kv[0, h], kv[1, h], wg[h], wu[h], wo[h], grad, h)
        both(h, "start")

    has_before = sum(lax.axis_index(axis) for axis in CTX) > 0
    has_after = sum(lax.axis_index(axis) for axis in CTX) < 9

    def attend(h):
        halo("receive", h)
        for j in range(3):
            sent[h, j, 2].wait_recv()
        attention(q_all.at[h], before.at[:, h], kv.at[:, h], after.at[:, h], attended.at[h], has_before, has_after)

    outs = {}

    def learn(h):
        update(total, weights, fresh, h)
        q = q_all[h]
        gate = dot(q, fresh[0])
        hid = (gate * jax.nn.sigmoid(gate) * dot(q, fresh[1])).astype(BF16)
        mixed[h] = (attended[h] + dot(hid, fresh[2])).astype(BF16)
        for j, p in enumerate(heads):
            outs[h, j] = copies.start(place(mixed.at[h], p), out_ref.at[:, cols(g, h)], {"head": p})
        out_ref[:, cols(g, h)] = mixed[h, pl.ds(pl.multiple_of(g * 128, 128), 128), :]

    head_in(0)
    both(0, "middle")
    head_in(1)
    both(0, "start2")
    both(1, "middle")
    both(0, "middle")
    both(1, "start2")
    both(0, "start3")
    both(1, "middle")
    both(1, "start3")
    halo("send", 1)
    both(0, "gather3")
    both(1, "gather3")
    both(0, "gather2")
    both(1, "gather2")
    halo("relay", 0)
    both(0, "middle")
    both(1, "middle")
    halo("relay", 1)
    both(0, "gather1")
    both(1, "gather1")
    halo("relay2", 0)
    both(0, "middle")
    halo("relay2", 1)
    both(1, "middle")
    halo("relay2_y")
    attend(0)
    both(0, "end")
    learn(0)
    attend(1)
    both(1, "end")
    learn(1)
    for copy in outs.values():
        copy.wait_recv()
    for copy in copies.all:
        copy.wait_send()
    halo("finish")


def per_device(queries, keys, values, w_gate, w_up, w_out):
    anywhere = pl.BlockSpec(memory_space=pl.ANY)
    n_copies = 174
    wide, matrices = (2, HD, HD), (3, HD, HD)
    return pl.pallas_call(
        kernel,
        out_shape=jax.ShapeDtypeStruct((128, 4096), BF16),
        in_specs=[anywhere] * 6,
        out_specs=pl.BlockSpec(memory_space=pltpu.VMEM),
        scratch_shapes=[
            pltpu.VMEM(wide, BF16),
            pltpu.VMEM(wide, BF16),
            pltpu.VMEM(wide, BF16),
            pltpu.VMEM(wide, BF16),
            pltpu.VMEM((2,) + wide, BF16),
            pltpu.VMEM((2,) + wide, BF16),
            pltpu.VMEM((2,) + wide, BF16),
            pltpu.VMEM((2,) + wide, BF16),
            pltpu.VMEM(wide, F32),
            pltpu.VMEM(wide, BF16),
            pltpu.VMEM(matrices, BF16),
            pltpu.VMEM((4, 3, 1024, 128), BF16),
            pltpu.VMEM((4, 2, 3, 128, 128), BF16),
            pltpu.VMEM((4, 2, 3, 256, 128), BF16),
            pltpu.VMEM((4, 3, 256, 128), F32),
            pltpu.VMEM((4, 2, 3, 32, 128), F32),
            pltpu.VMEM((4, 2, 3, 64, 128), F32),
            pltpu.VMEM((4, 3, 64, 128), F32),
            pltpu.VMEM((4, 3, 3, 16, 128), F32),
            pltpu.VMEM((4, 3, 1024, 128), BF16),
            pltpu.SemaphoreType.DMA((n_copies,)),
            pltpu.SemaphoreType.DMA((n_copies,)),
            pltpu.SemaphoreType.DMA((9,)),
        ],
        compiler_params=pltpu.CompilerParams(
            collective_id=0, has_side_effects=True, vmem_limit_bytes=56 * 1024 * 1024
        ),
        name="layer",
    )(queries, keys, values, w_gate, w_up, w_out)


def solution(mesh):
    split = Mesh(mesh.devices.reshape(4, 4, 4, 4), ("head", Y, Z, X))
    rows_spec, heads_spec = P(CTX_HEAD, None), P("head", None, None)
    return jax.shard_map(
        per_device,
        mesh=split,
        in_specs=(rows_spec,) * 3 + (heads_spec,) * 3,
        out_specs=rows_spec,
        check_vma=False,
    )
```

```python
import jax
import jax.numpy as jnp
from jax import lax
from jax.experimental import pallas as pl
from jax.experimental.pallas import tpu as pltpu
from jax.sharding import Mesh
from jax.sharding import PartitionSpec as P

HD = 512
WIN = 512
Y, Z, X = "ctx_0", "ctx_1", "ctx_2"
CTX = (Y, Z, X)
CTX_HEAD = CTX + ("head",)
MESH = pl.DeviceIdType.MESH
STEP = 0.02
EPS = 1e-06
F32, BF16 = jnp.float32, jnp.bfloat16


def dot(a, b, dims=((1,), (0,))):
    return lax.dot_general(a, b, (dims, ((), ())), preferred_element_type=F32)


class Copies:
    def __init__(self, send_sem, recv_sem):
        self.send_sem, self.recv_sem, self.count, self.all = send_sem, recv_sem, 0, []

    def make(self, src, dst, device):
        copy = pltpu.make_async_remote_copy(
            src_ref=src,
            dst_ref=dst,
            send_sem=self.send_sem.at[self.count],
            recv_sem=self.recv_sem.at[self.count],
            device_id=device,
            device_id_type=MESH,
        )
        self.count += 1
        return copy

    def start(self, src, dst, device):
        copy = self.make(src, dst, device)
        self.all.append(copy)
        copy.start()
        return copy


def ring(axis):
    me = lax.axis_index(axis)
    return me, lax.rem(me + 1, 4), lax.rem(me + 3, 4), lax.rem(me + 2, 4)


def rows(base, index, size, part=0, parts=1):
    step = size // parts
    return pl.ds(pl.multiple_of(base + index * size + part * step, 16), step)


def add_into(buf, at, other):
    buf[:, at, :] = (buf[:, at, :].astype(F32) + other.astype(F32)).astype(buf.dtype)


class RingReduce:
    def __init__(self, copies, axis, buf, c, opp, side):
        self.copies, self.axis, self.buf, self.c, self.opp, self.side = copies, axis, buf, c, opp, side
        me, right, left, far = ring(axis)
        half = c // 2
        r, l = {axis: right}, {axis: left}
        self.far_r = copies.start(buf.at[:, rows(0, far, c, 0, 2), :], opp.at[0], r)
        self.far_l = copies.start(buf.at[:, rows(0, far, c, 1, 2), :], opp.at[1], l)
        self.near_r = copies.start(buf.at[:, rows(0, right, c, 1, 2), :], side.at[0, :, pl.ds(half, half), :], r)
        self.near_l = copies.start(buf.at[:, rows(0, left, c, 0, 2), :], side.at[1, :, pl.ds(0, half), :], l)

    def middle(self):
        me, right, left, far = ring(self.axis)
        c, buf, half = self.c, self.buf, self.c // 2
        self.far_r.wait_recv()
        at = rows(0, right, c, 0, 2)
        add_into(buf, at, self.opp[0])
        self.last_r = self.copies.start(buf.at[:, at, :], self.side.at[0, :, pl.ds(0, half), :], {self.axis: right})
        self.far_l.wait_recv()
        at = rows(0, left, c, 1, 2)
        add_into(buf, at, self.opp[1])
        self.last_l = self.copies.start(buf.at[:, at, :], self.side.at[1, :, pl.ds(half, half), :], {self.axis: left})

    def end(self, out):
        me = lax.axis_index(self.axis)
        for copy in (self.near_r, self.near_l, self.last_r, self.last_l):
            copy.wait_recv()
        own = self.buf[:, rows(0, me, self.c), :].astype(F32)
        out[...] = own + self.side[0].astype(F32) + self.side[1].astype(F32)


class LineReduce:
    def __init__(self, copies, axis, buf, c, slots):
        me = lax.axis_index(axis)
        self.axis, self.buf, self.c, self.slots, self.sent = axis, buf, c, slots, []
        for d in (1, 2, 3):
            peer = lax.rem(me + d, 4)
            self.sent.append(copies.start(buf.at[:, rows(0, peer, c), :], slots.at[d - 1], {axis: peer}))

    def end(self):
        total = self.buf[:, rows(0, lax.axis_index(self.axis), self.c), :]
        for d in range(3):
            self.sent[d].wait_recv()
            total += self.slots[d]
        return total


class LineGather:
    def __init__(self, copies, axis, buf, base, c):
        me = lax.axis_index(axis)
        at = buf.at[:, rows(base, me, c), :]
        self.sent = [copies.start(at, at, {axis: lax.rem(me + d, 4)}) for d in (1, 2, 3)]

    def end(self):
        for copy in self.sent:
            copy.wait_recv()


class RingGather:
    def __init__(self, copies, axis, buf, base, c):
        self.copies, self.axis, self.buf, self.base, self.c = copies, axis, buf, base, c
        me, right, left, far = ring(axis)
        low, high = (buf.at[:, rows(base, me, c, part, 2), :] for part in (0, 1))
        self.low_r = copies.start(low, low, {axis: right})
        self.high_l = copies.start(high, high, {axis: left})
        self.high_r = copies.start(high, high, {axis: right})
        self.low_l = copies.start(low, low, {axis: left})

    def middle(self):
        me, right, left, far = ring(self.axis)
        self.low_r.wait_recv()
        at = self.buf.at[:, rows(self.base, left, self.c, 0, 2), :]
        self.far_r = self.copies.start(at, at, {self.axis: right})
        self.high_l.wait_recv()
        at = self.buf.at[:, rows(self.base, right, self.c, 1, 2), :]
        self.far_l = self.copies.start(at, at, {self.axis: left})

    def end(self):
        for copy in (self.high_r, self.low_l, self.far_r, self.far_l):
            copy.wait_recv()


class Group:
    def __init__(self, copies, g, bufs):
        self.copies, self.g = copies, g
        self.first, self.second = (Y, X)
        self.b = {name: ref.at[g] for name, ref in bufs.items()}
        self.base = lax.axis_index(self.first) * 256
        self.inner = self.base + lax.axis_index(self.second) * 64

    def start(self):
        b = self.b
        self.now = RingReduce(self.copies, self.first, b["grad"], 256, b["opp1"], b["side1"])

    def middle(self):
        self.now.middle()

    def start2(self):
        b = self.b
        self.now.end(b["part2"])
        self.now = RingReduce(self.copies, self.second, b["part2"], 64, b["opp2"], b["side2"])

    def start3(self):
        b = self.b
        self.now.end(b["part3"])
        self.now = LineReduce(self.copies, Z, b["part3"], 16, b["slots"])

    def gather3(self):
        b = self.b
        b["total"][:, rows(self.inner, lax.axis_index(Z), 16), :] = self.now.end().astype(BF16)
        self.now = LineGather(self.copies, Z, b["total"], self.inner, 16)

    def gather2(self):
        self.now.end()
        self.now = RingGather(self.copies, self.second, self.b["total"], self.base, 64)

    def gather1(self):
        self.now.end()
        self.now = RingGather(self.copies, self.first, self.b["total"], 0, 256)

    def end(self):
        self.now.end()


def gradients(k, v, wg, wu, wo, grad, h):
    a, b = dot(k, wg), dot(k, wu)
    back = -dot(v, wo, ((1,), (1,)))
    sig = jax.nn.sigmoid(a)
    act = a * sig
    hidden = (act * b).astype(BF16)
    da = (back * b * (sig * (1.0 + a * (1.0 - sig)))).astype(BF16)
    db = (back * act).astype(BF16)
    pairs = ((k, da), (k, db), (hidden, v))
    for m, (left, right) in enumerate(pairs):
        g = dot(left, right, ((0,), (0,)))
        g = -g if m == 2 else g
        for part in range(4):
            at = pl.ds((part % 2) * HD, HD)
            grad[2 * h + part // 2, m, at, :] = g[:, part * 128 : part * 128 + 128].astype(BF16)


def update(total, weights, fresh, h):
    for m, w_ref in enumerate(weights):
        squares = 0.0
        for color in range(2):
            g = total[2 * h + color, m].astype(F32)
            squares += jnp.sum(g * g)
        scale = STEP * lax.rsqrt(squares / (HD * HD) + EPS)
        for part in range(4):
            cols = pl.ds(part * 128, 128)
            g = total[2 * h + part // 2, m, pl.ds((part % 2) * HD, HD), :].astype(F32)
            fresh[m, :, cols] = (w_ref[h, :, cols].astype(F32) - scale * g).astype(BF16)


def attention(q_ref, before, own, after, out, has_before, has_after):
    r = lax.broadcasted_iota(jnp.int32, (256, 256), 0)
    c = lax.broadcasted_iota(jnp.int32, (256, 256), 1)
    for t in range(2):
        top = pl.ds(t * 256, 256)
        q = q_ref[top, :]
        nb = 512 - t * 256
        late, early = pl.ds(t * 256, nb), pl.ds(0, 256 + t * 256)
        sb = dot(q, before[0, late, :], ((1,), (1,))) * HD**-0.5
        so = dot(q, own[0], ((1,), (1,))) * HD**-0.5
        sa = dot(q, after[0, early, :], ((1,), (1,))) * HD**-0.5
        pieces = [jnp.where((c >= r) & has_before, sb[:, :256], -1e30)]
        if t == 0:
            pieces += [jnp.where(has_before, sb[:, 256:], -1e30), so]
        else:
            pieces += [so, jnp.where(has_after, sa[:, :256], -1e30)]
        pieces.append(jnp.where((c <= r) & has_after, sa[:, t * 256 :], -1e30))
        s = jnp.concatenate(pieces, axis=1)
        s = jnp.exp(s - jnp.max(s, axis=1, keepdims=True))
        p = (s / jnp.sum(s, axis=1, keepdims=True)).astype(BF16)
        o = dot(p[:, :nb], before[1, late, :]) + dot(p[:, nb : nb + 512], own[1])
        out[top, :] = o + dot(p[:, nb + 512 :], after[1, early, :])


class Halo:
    def __init__(self, copies, kv, dst, relays, delta, hi):
        x, y, z = (lax.axis_index(axis) for axis in (X, Y, Z))
        self.source, self.last = (3, 0) if delta == 1 else (0, 3)
        self.x = x
        self.is_source, self.is_last = x == self.source, x == self.last
        row = lax.rem(y * 4 + z + delta + 16, 16)
        ahead = {Y: row // 4, Z: lax.rem(row, 4)}
        nearby = {X: lax.rem(x + delta + 4, 4)}
        every = slice(None)
        own = pl.ds(pl.multiple_of(hi * 256, 256), 256)
        other = pl.ds(pl.multiple_of((1 - hi) * 256, 256), 256)
        self.early = copies.make(kv.at[:, :, own, :], dst.at[:, :, own, :], nearby)
        self.cross = [copies.make(kv.at[:, h, other, :], dst.at[:, h, other, :], nearby) for h in range(2)]
        self.leg1, self.leg2, self.leg3 = {}, {}, {}
        for c in range(4):
            piece, end = kv.at[c % 2, c // 2], dst.at[c % 2, c // 2]
            if c != self.source:
                self.leg1[c] = copies.make(piece, relays.at[0], {X: jnp.int32(c)})
                piece = relays.at[0]
            self.leg2[c] = copies.make(piece, end if c == self.last else relays.at[1], ahead)
            if c != self.last:
                self.leg3[c] = copies.make(relays.at[1], end, {X: jnp.int32(self.last)})

    def send_early(self):
        pl.when(jnp.logical_not(self.is_source))(self.early.start)

    def send(self, h):
        pl.when(jnp.logical_not(self.is_source))(self.cross[h].start)

        @pl.when(self.is_source)
        def _():
            for c in (2 * h, 2 * h + 1):
                if c != self.source:
                    self.leg1[c].start()

    def relay(self, h):
        for c in (2 * h, 2 * h + 1):
            if c != self.source:
                pl.when(self.x == c)(self.leg1[c].wait_recv)
            pl.when(self.x == c)(self.leg2[c].start)

    def relay2(self, h):
        for c in (2 * h, 2 * h + 1):
            if c != self.last:

                @pl.when(self.x == c)
                def _():
                    self.leg2[c].wait_recv()
                    self.leg3[c].start()

    def receive(self, h):
        for c in (2 * h, 2 * h + 1):
            pl.when(self.is_last)((self.leg2 if c == self.last else self.leg3)[c].wait_recv)

        @pl.when(jnp.logical_not(self.is_last))
        def _():
            if h == 0:
                self.early.wait_recv()
            self.cross[h].wait_recv()

    def finish(self):
        @pl.when(jnp.logical_not(self.is_source))
        def _():
            self.early.wait_send()
            for h in range(2):
                self.cross[h].wait_send()

        @pl.when(self.is_source)
        def _():
            for copy in self.leg1.values():
                copy.wait_send()

        for c in range(4):
            pl.when(self.x == c)(self.leg2[c].wait_send)
            if c != self.last:
                pl.when(self.x == c)(self.leg3[c].wait_send)


def kernel(
    q_in, k_in, v_in, wg_in, wu_in, wo_in, out_ref,
    wg, wu, wo, q_all, kv, before, after, relays, attended, mixed, fresh,
    grad, opp1, side1, part2, opp2, side2, part3, slots, total, send_sem, recv_sem, local_sem,
):
    g = lax.axis_index("head")
    hi, core = g // 2, lax.rem(g, 2)
    heads = ((1 - hi) * 2 + core, (1 - hi) * 2 + 1 - core, hi * 2 + 1 - core)
    barrier = pltpu.get_barrier_semaphore()
    partners = [{"head": p} for p in heads]
    for axis, offsets in ((X, (1, 2, 3)), (Y, (1, 3)), (Z, (1, 2, 3))):
        partners += [{axis: lax.rem(lax.axis_index(axis) + d, 4)} for d in offsets]
    for d in (1, 3):
        partners.append({axis: lax.rem(lax.axis_index(axis) + d, 4) for axis in (Y, Z)})
    for p in partners:
        pl.semaphore_signal(barrier, inc=1, device_id=p, device_id_type=MESH)
    def cols(p, h):
        return pl.ds(pl.multiple_of(p * 1024 + h * HD, HD), HD)

    def place(ref, p):
        return ref.at[pl.ds(pl.multiple_of(p * 128, 128), 128), :]

    local = []

    def stay(src, dst):
        copy = pltpu.make_async_copy(src, dst, local_sem.at[len(local)])
        copy.start()
        local.append(copy)

    for h in range(2):
        for i, ref in enumerate((k_in, v_in)):
            stay(ref.at[:, cols(g, h)], place(kv.at[i, h], g))
        stay(q_in.at[:, cols(g, h)], place(q_all.at[h], g))
    for src, dst in ((wg_in, wg), (wu_in, wu), (wo_in, wo)):
        stay(src, dst)

    copies = Copies(send_sem, recv_sem)
    pl.semaphore_wait(barrier, len(partners))
    sent = {}

    def send_pairs(h, js):
        for j in js:
            for i, ref in enumerate((k_in, v_in)):
                sent[h, j, i] = copies.start(ref.at[:, cols(heads[j], h)], place(kv.at[i, h], g), {"head": heads[j]})

    send_pairs(0, (0, 1, 2))
    send_pairs(1, (2,))

    def send_queries(h):
        for j, p in enumerate(heads):
            sent[h, j, 2] = copies.start(q_in.at[:, cols(p, h)], place(q_all.at[h], g), {"head": p})

    halos = [Halo(copies, kv, dst, relays.at[j], delta, hi) for j, (dst, delta) in enumerate(((before, 1), (after, -1)))]

    def halo(step, *args):
        for h in halos:
            getattr(h, step)(*args)

    for copy in local:
        copy.wait()
    for h in range(2):
        for i in range(2):
            sent[h, 2, i].wait_recv()
    halo("send_early")

    bufs = dict(
        grad=grad, opp1=opp1, side1=side1, part2=part2, opp2=opp2, side2=side2, part3=part3, slots=slots, total=total
    )
    groups = [Group(copies, n, bufs) for n in range(4)]
    weights = (wg, wu, wo)

    def both(h, step):
        for group in groups[2 * h : 2 * h + 2]:
            getattr(group, step)()

    def head_in(h):
        for j in range(2):
            for i in range(2):
                sent[h, j, i].wait_recv()
        if h == 0:
            send_pairs(1, (0, 1))
            halo("send", 0)
        else:
            send_queries(0)
            send_queries(1)
        gradients(kv[0, h], kv[1, h], wg[h], wu[h], wo[h], grad, h)
        both(h, "start")

    has_before = sum(lax.axis_index(axis) for axis in CTX) > 0
    has_after = sum(lax.axis_index(axis) for axis in CTX) < 9

    def attend(h):
        halo("receive", h)
        for j in range(3):
            sent[h, j, 2].wait_recv()
        attention(q_all.at[h], before.at[:, h], kv.at[:, h], after.at[:, h], attended.at[h], has_before, has_after)

    outs = {}

    def learn(h):
        update(total, weights, fresh, h)
        q = q_all[h]
        gate = dot(q, fresh[0])
        hid = (gate * jax.nn.sigmoid(gate) * dot(q, fresh[1])).astype(BF16)
        mixed[h] = (attended[h] + dot(hid, fresh[2])).astype(BF16)
        for j, p in enumerate(heads):
            outs[h, j] = copies.start(place(mixed.at[h], p), out_ref.at[:, cols(g, h)], {"head": p})
        out_ref[:, cols(g, h)] = mixed[h, pl.ds(pl.multiple_of(g * 128, 128), 128), :]

    head_in(0)
    both(0, "middle")
    head_in(1)
    both(0, "start2")
    both(1, "middle")
    both(0, "middle")
    both(1, "start2")
    both(0, "start3")
    both(1, "middle")
    both(1, "start3")
    halo("send", 1)
    both(0, "gather3")
    both(1, "gather3")
    both(0, "gather2")
    both(1, "gather2")
    halo("relay", 0)
    both(0, "middle")
    both(1, "middle")
    halo("relay", 1)
    both(0, "gather1")
    both(1, "gather1")
    halo("relay2", 0)
    both(0, "middle")
    both(1, "middle")
    halo("relay2", 1)
    attend(0)
    both(0, "end")
    learn(0)
    attend(1)
    both(1, "end")
    learn(1)
    for copy in outs.values():
        copy.wait_recv()
    for copy in copies.all:
        copy.wait_send()
    halo("finish")


def per_device(queries, keys, values, w_gate, w_up, w_out):
    anywhere = pl.BlockSpec(memory_space=pl.ANY)
    n_copies = 174
    wide, matrices = (2, HD, HD), (3, HD, HD)
    return pl.pallas_call(
        kernel,
        out_shape=jax.ShapeDtypeStruct((128, 4096), BF16),
        in_specs=[anywhere] * 6,
        out_specs=pl.BlockSpec(memory_space=pltpu.VMEM),
        scratch_shapes=[
            pltpu.VMEM(wide, BF16),
            pltpu.VMEM(wide, BF16),
            pltpu.VMEM(wide, BF16),
            pltpu.VMEM(wide, BF16),
            pltpu.VMEM((2,) + wide, BF16),
            pltpu.VMEM((2,) + wide, BF16),
            pltpu.VMEM((2,) + wide, BF16),
            pltpu.VMEM((2,) + wide, BF16),
            pltpu.VMEM(wide, F32),
            pltpu.VMEM(wide, BF16),
            pltpu.VMEM(matrices, BF16),
            pltpu.VMEM((4, 3, 1024, 128), BF16),
            pltpu.VMEM((4, 2, 3, 128, 128), BF16),
            pltpu.VMEM((4, 2, 3, 256, 128), BF16),
            pltpu.VMEM((4, 3, 256, 128), F32),
            pltpu.VMEM((4, 2, 3, 32, 128), F32),
            pltpu.VMEM((4, 2, 3, 64, 128), F32),
            pltpu.VMEM((4, 3, 64, 128), F32),
            pltpu.VMEM((4, 3, 3, 16, 128), F32),
            pltpu.VMEM((4, 3, 1024, 128), BF16),
            pltpu.SemaphoreType.DMA((n_copies,)),
            pltpu.SemaphoreType.DMA((n_copies,)),
            pltpu.SemaphoreType.DMA((9,)),
        ],
        compiler_params=pltpu.CompilerParams(
            collective_id=0, has_side_effects=True, vmem_limit_bytes=56 * 1024 * 1024
        ),
        name="layer",
    )(queries, keys, values, w_gate, w_up, w_out)


def solution(mesh):
    split = Mesh(mesh.devices.reshape(4, 4, 4, 4), ("head", Y, Z, X))
    rows_spec, heads_spec = P(CTX_HEAD, None), P("head", None, None)
    return jax.shard_map(
        per_device,
        mesh=split,
        in_specs=(rows_spec,) * 3 + (heads_spec,) * 3,
        out_specs=rows_spec,
        check_vma=False,
    )
```
